256 devices in a mesh: pool: 8 (over y, core), expert: 32 (over x, z).
Axes of the slice: x: 4, y: 4, z: 8, core: 2. Of those that a mesh axis runs over, the one named last changes fastest.
Arguments:
- residual: bfloat16 [256, 2, 4096], P('expert'), may hold values from -6 to 6
- queries: bfloat16 [256, 2, 32, 128], P('expert', None, 'pool'), may hold values from -150 to 150
- kv_cache: bfloat16 [256, 512, 2, 2, 128], P('expert'), may hold values from -6 to 6
- kv_pages: bfloat16 [32, 32, 64, 2, 2, 128], P('pool', 'expert'), may hold values from -6 to 6
- cache_len: int32 [256], P('expert'), may hold values from 1 to 510, 65280 in all
- page_row: int32 [32, 32], P(None, 'expert'), may hold values from 0 to 7
- page_len: int32 [32, 32], P(None, 'expert'), may hold values from 1 to 64
- routes: int32 [256, 2, 8], P('expert'), may hold values from 0 to 63, all different within a row; in each aligned block of 16 rows (0 to 15, 16 to 31, ..., all dimensions but the last counted through in order) at most 3 rows name the same one
- route_weight: float32 [256, 2, 8], P('expert'), may hold values from 0.05 to 0.5
- out_weight: bfloat16 [4096, 4096], P('pool'), may hold values from -1.5 to 1.5
- gate_weight: bfloat16 [64, 4096, 1024], P('expert', None, 'pool'), may hold values from -0.09375 to 0.09375
- up_weight: bfloat16 [64, 4096, 1024], P('expert', None, 'pool'), may hold values from -0.09375 to 0.09375
- down_weight: bfloat16 [64, 1024, 4096], P('expert', 'pool'), may hold values from -0.375 to 0.375
Outputs:
- layer_out: bfloat16 [256, 2, 4096], P('expert')
The draws below stay inside these ranges and needn't reach their ends.
Inputs may be any that keep to these rules, and one draw needn't show every extreme that they name: The row's two new tokens sit at positions cache_len and cache_len + 1 of its cache. The page belongs to row e * 8 + page_row of its group e. `routes`: a token names distinct experts; among the 16 new tokens of one device's rows no expert is named by more than 3 tokens.
All inputs are finite; a program needn't handle non-finite values. No bound on the sum of `cache_len` on one device may be relied on, other than what follows from the above.
Results may differ from the reference program's by a relative error of at most 0.028.
Values may be sent and summed in bfloat16 or wider, within the bound.
A program may use at most 64 MiB of HBM per device.

```python
import math
import jax
import jax.numpy as jnp
import numpy as np
from jax import lax

D = 4096
QH = 32
KVH = 2
HD = 128
FF = 1024
TOP = 8
R_DEV = 8
LMAX = 512
PAGE = 64
ROWS = 256
EXPERTS = 64
SLOTS = 32
CAP = 3
N_POOL = 8
N_EXPERT = 32


def cache_numbers(key):
    base = jax.random.truncated_normal(jax.random.fold_in(key, 11), -6.0, 6.0, (ROWS, LMAX, KVH, 2, HD), jnp.float32)
    return base


def draw_kv_cache(key, part):
    return cache_numbers(key).astype(jnp.bfloat16)


def draw_queries(key, part):
    base = jax.random.truncated_normal(jax.random.fold_in(key, 23), -6.0, 6.0, (ROWS, 2, QH, HD), jnp.float32)
    return base.astype(jnp.bfloat16)


def set_ends(drawn, rng, low, top_value):
    spot = [jax.random.randint(jax.random.fold_in(rng, axis), (), 0, length) for axis, length in enumerate(drawn.shape)]
    widest = drawn.shape.index(max(drawn.shape))
    next_to = spot[:widest] + [(spot[widest] + 1) % drawn.shape[widest]] + spot[widest + 1:]
    return drawn.at[tuple(spot)].set(low).at[tuple(next_to)].set(top_value)


def steps_of(stream_key, shape, split, least, largest):
    level = 1.0
    for dim, parts in split:
        draws = jax.random.uniform(jax.random.fold_in(jax.random.fold_in(stream_key, 6), dim), (parts,), jnp.float32, least / len(split), largest / len(split))
        level = level * jnp.repeat(jnp.exp(draws), shape[dim] // parts).reshape((-1,) + (1,) * (len(shape) - 1 - dim))
    return level


def length_profile(amount, total, most, lean):
    weights = [(1 << 20) // math.isqrt(rank ** lean) + 1 for rank in range(2, amount + 1)]
    surplus, holding = total - most - (amount - 1), [1] * (amount - 1)
    while surplus > 0:
        movable = [i for i in range(amount - 1) if holding[i] < most]
        mass, left = sum([weights[i] for i in movable]), surplus
        for i in movable:
            more = min(most - holding[i], max(1, left * weights[i] // mass), surplus)
            holding[i] = holding[i] + more
            surplus = surplus - more
    return np.array([most] + holding)


def ragged_sizes(stream_key, count, total, limit, skew):
    if count == 2:
        one = jax.random.randint(stream_key, (), max(1, total - limit), min(limit, total - 1) + 1)
        return jnp.stack([one, total - one])
    tallies = jnp.asarray(length_profile(count, total, limit, skew), jnp.int32)
    couples = (count - 1) // 2
    giver, taker = tallies[1:1 + 2 * couples:2], tallies[2:2 + 2 * couples:2]
    room = jnp.minimum(giver - 1, limit - taker)
    moved = jax.random.randint(jax.random.fold_in(stream_key, 1), (couples,), 0, 1 << 20) % (room + 1)
    tallies = tallies.at[1:1 + 2 * couples:2].set(giver - moved).at[2:2 + 2 * couples:2].set(taker + moved)
    return tallies[jax.random.permutation(jax.random.fold_in(stream_key, 2), count)]


def shared_out(key, own, number, rows, count, top, bound, slope):
    order = jax.random.permutation(key, count)
    packed, common = portions_of(count, rows * top, bound, slope, True), portions_of(count, rows * top, bound, slope, False)
    places = jnp.arange(count)

    def named(sizes, rotation):
        used = int((sizes > 0).sum())
        fixed = max(1, used // 4)
        passed = fixed + (places - fixed + rotation * (used - fixed)) % max(1, count - fixed)
        return jnp.zeros((count,), jnp.int32).at[order[jnp.where(places < fixed, places, passed)]].set(jnp.asarray(sizes, jnp.int32))

    sizes = jnp.where(number % 4 == 0, named(packed, number // 4), named(common, number - number // 4 - 1))
    mixed = jax.random.permutation(jax.random.fold_in(own, 3), count)
    donor, taker = mixed[0:count // 2 * 2:2], mixed[1:count // 2 * 2:2]
    margin = jnp.minimum(sizes[donor] - 1, bound - sizes[taker]) // 2
    margin = jnp.where((donor == order[0]) | (taker == order[0]) | (sizes[taker] == 0), 0, jnp.maximum(margin, 0))
    passed = jax.random.randint(jax.random.fold_in(own, 4), (count // 2,), 0, 1 << 20) % (margin + 1)
    sizes = sizes.at[donor].add(-passed).at[taker].add(passed)
    labels = jnp.searchsorted(jnp.cumsum(sizes), jnp.arange(rows * top), side="right").astype(jnp.int32)
    table = labels.reshape(top, rows).T
    table = table[jax.random.permutation(jax.random.fold_in(own, 1), rows)]
    rotation = jax.random.randint(jax.random.fold_in(own, 2), (rows, 1), 0, top)
    return jnp.take_along_axis(table, (jnp.arange(top)[None, :] + rotation) % top, axis=1)


def portions_of(count, total, most, skew, full):
    weights = [(1 << 20) // math.isqrt(standing ** skew) + 1 for standing in range(1, count + 1)]
    largest = most if full else min(most, max(-(-total // count), total * weights[0] // sum(weights)))
    least = 1 if total - largest >= count - 1 else 0
    counts, surplus = [largest] + [least] * (count - 1), total - largest - least * (count - 1)
    while surplus > 0:
        movable = [i for i in range(1, count) if counts[i] < largest] or [i for i in range(1, count) if counts[i] < most]
        pool, remaining = sum([weights[i] for i in movable]), surplus
        for i in movable:
            extra = min(most - counts[i], max(1, remaining * weights[i] // pool), surplus)
            counts[i] = counts[i] + extra
            surplus = surplus - extra
    return np.array(counts)


def normal_values(key, extent, width, reach, shards=(), kind=jnp.bfloat16):
    values = width * jax.random.normal(key, extent, jnp.float32)
    if shards:
        values = values * steps_of(key, extent, shards, -0.22, 0.18)
    return jnp.clip(values, -reach, reach).astype(kind)


def setup_inputs(seed: int = 0) -> dict:
    key_list = jax.random.split(jax.random.key(seed), 14)
    residual = normal_values(key_list[0], (ROWS, 2, D), 1.0, 6.0, ((0, 32),))
    queries = draw_queries(jax.random.fold_in(key_list[13], 71), 0)
    kv_cache = draw_kv_cache(jax.random.fold_in(key_list[13], 71), 0)
    kv_pages = normal_values(key_list[3], (SLOTS, N_EXPERT, PAGE, KVH, 2, HD), 1.0, 6.0, ((0, 8), (1, 32)))
    cache_len = ragged_sizes(key_list[4], ROWS, ROWS * (LMAX - 2) // 2, LMAX - 2, 2).astype(jnp.int32)
    page_row = set_ends(jax.random.randint(key_list[5], (SLOTS, N_EXPERT), 0, R_DEV), jax.random.fold_in(key_list[5], 1), 0, R_DEV - 1).astype(jnp.int32)
    page_len = set_ends(jax.random.randint(key_list[6], (SLOTS, N_EXPERT), 1, PAGE + 1), jax.random.fold_in(key_list[6], 1), 1, PAGE).astype(jnp.int32)
    routes_keys = jax.random.split(jax.random.fold_in(key_list[7], 1), ROWS * 2 // (2 * R_DEV))
    routes_turns = jax.random.permutation(jax.random.fold_in(key_list[7], 3), ROWS * 2 // (2 * R_DEV))
    routes = jax.vmap(lambda own, number: shared_out(jax.random.fold_in(key_list[7], 2), own, number, 2 * R_DEV, EXPERTS, TOP, CAP, 2))(routes_keys, routes_turns).reshape((ROWS, 2, TOP))
    route_weight = jnp.clip(jnp.exp(math.log(0.5) - 2.3025851 * jax.random.uniform(key_list[8], (ROWS, 2, TOP), jnp.float32) ** steps_of(key_list[8], (ROWS, 2, TOP), ((0, 32),), -0.2, 0.2)), 0.05, 0.5)
    out_weight = normal_values(key_list[9], (QH * HD, D), 16 ** -0.5, 1.5, ((0, 8),))
    gate_weight = normal_values(key_list[10], (EXPERTS, D, FF), D ** -0.5, 0.09375, ((0, 32), (2, 8)))
    up_weight = normal_values(key_list[11], (EXPERTS, D, FF), D ** -0.5, 0.09375, ((0, 32), (2, 8)))
    down_weight = normal_values(key_list[12], (EXPERTS, FF, D), (FF // 4) ** -0.5, 0.375, ((0, 32), (1, 8)))
    return {"residual": residual, "queries": queries, "kv_cache": kv_cache, "kv_pages": kv_pages, "cache_len": cache_len, "page_row": page_row, "page_len": page_len, "routes": routes, "route_weight": route_weight, "out_weight": out_weight, "gate_weight": gate_weight, "up_weight": up_weight, "down_weight": down_weight}


def attend_group(operands):
    group_queries, group_cache, group_lens, group_pages, group_rows, group_sizes = operands
    heads_per = QH // KVH
    score_scale = 1.0 / (HD ** 0.5)
    grouped = group_queries.astype(jnp.float32).reshape(R_DEV, 2, KVH, heads_per, HD)
    cache_keys = group_cache[:, :, :, 0].astype(jnp.float32)
    cache_values = group_cache[:, :, :, 1].astype(jnp.float32)
    page_keys = group_pages[:, :, :, 0].astype(jnp.float32).reshape(SLOTS * PAGE, KVH, HD)
    page_values = group_pages[:, :, :, 1].astype(jnp.float32).reshape(SLOTS * PAGE, KVH, HD)
    cache_scores = jnp.einsum("rtgjd,rlgd->rtgjl", grouped, cache_keys) * score_scale
    page_scores = jnp.einsum("rtgjd,kgd->rtgjk", grouped, page_keys) * score_scale
    last_seen = group_lens[:, None] + jnp.arange(2, dtype=jnp.int32)[None, :]
    cache_allowed = (jnp.arange(LMAX, dtype=jnp.int32)[None, None, :] <= last_seen[:, :, None])[:, :, None, None, :]
    token_allowed = jnp.arange(PAGE, dtype=jnp.int32)[None, :] < group_sizes[:, None]
    page_allowed = (group_rows[None, :, None] == jnp.arange(R_DEV, dtype=jnp.int32)[:, None, None]) & token_allowed[None]
    page_allowed = page_allowed.reshape(R_DEV, 1, 1, 1, SLOTS * PAGE)
    scores = jnp.concatenate([cache_scores, page_scores], axis=-1)
    allowed = jnp.concatenate([jnp.broadcast_to(cache_allowed, cache_scores.shape), jnp.broadcast_to(page_allowed, page_scores.shape)], axis=-1)
    row_top = jnp.max(jnp.where(allowed, scores, -1e30), axis=-1, keepdims=True)
    weights = jnp.where(allowed, jnp.exp(scores - row_top), 0.0)
    row_total = jnp.sum(weights, axis=-1)
    rounded = lax.optimization_barrier(weights.astype(jnp.bfloat16)).astype(jnp.float32)
    mixed_sum = jnp.einsum("rtgjl,rlgd->rtgjd", rounded[..., :LMAX], cache_values)
    mixed_sum = mixed_sum + jnp.einsum("rtgjk,kgd->rtgjd", rounded[..., LMAX:], page_values)
    attended = mixed_sum / row_total[..., None]
    return attended.reshape(R_DEV, 2, QH * HD).astype(jnp.bfloat16)


def reference(residual, queries, kv_cache, kv_pages, cache_len, page_row, page_len, routes, route_weight, out_weight, gate_weight, up_weight, down_weight):
    operands = (
        queries.reshape(N_EXPERT, R_DEV, 2, QH, HD),
        kv_cache.reshape(N_EXPERT, R_DEV, LMAX, KVH, 2, HD),
        cache_len.reshape(N_EXPERT, R_DEV),
        jnp.moveaxis(kv_pages, 1, 0),
        page_row.T,
        page_len.T,
    )
    attended = lax.map(attend_group, operands).reshape(ROWS * 2, QH * HD)
    projected = jnp.dot(attended, out_weight, preferred_element_type=jnp.float32)
    hidden = residual.reshape(ROWS * 2, D).astype(jnp.float32) + projected
    hidden_low = hidden.astype(jnp.bfloat16)
    flat_routes = routes.reshape(ROWS * 2, TOP)
    flat_weight = route_weight.reshape(ROWS * 2, TOP)
    capacity = CAP * N_EXPERT

    def expert_rows(expert_index):
        named = flat_routes == expert_index
        chosen = jnp.any(named, axis=1)
        weight = jnp.sum(jnp.where(named, flat_weight, 0.0), axis=1)
        members = jnp.nonzero(chosen, size=capacity, fill_value=0)[0].astype(jnp.int32)
        filled = jnp.arange(capacity, dtype=jnp.int32) < jnp.sum(chosen.astype(jnp.int32))
        inputs = hidden_low[members]
        gate_value = jnp.dot(inputs, gate_weight[expert_index], preferred_element_type=jnp.float32)
        up_value = jnp.dot(inputs, up_weight[expert_index], preferred_element_type=jnp.float32)
        active = (jax.nn.silu(gate_value) * up_value).astype(jnp.bfloat16)
        sliced = active.astype(jnp.float32).reshape(capacity, N_POOL, FF // N_POOL)
        down_slices = down_weight[expert_index].astype(jnp.float32).reshape(N_POOL, FF // N_POOL, D)
        partial_value = jnp.einsum("mpf,pfd->mpd", sliced, down_slices)
        pieces = lax.optimization_barrier(partial_value.astype(jnp.bfloat16)).astype(jnp.float32)
        summed = jnp.sum(pieces, axis=1)
        factor = jnp.where(filled, weight[members], 0.0)
        return members, summed * factor[:, None]

    members, contribution = lax.map(expert_rows, jnp.arange(EXPERTS, dtype=jnp.int32))
    expert_sum = jnp.zeros((ROWS * 2, D), jnp.float32).at[members.reshape(-1)].add(contribution.reshape(-1, D))
    return (hidden + expert_sum).astype(jnp.bfloat16).reshape(ROWS, 2, D)
```

```python
import functools
import math

import jax
import jax.numpy as jnp
from jax import lax
from jax.experimental import pallas as pl
from jax.experimental.pallas import tpu as pltpu
from jax.sharding import PartitionSpec as P

very_low = -1e30
MESH = pl.DeviceIdType.MESH
bf16, f32 = jnp.bfloat16, jnp.float32
POOL, EXPERT = 8, 32
CAP = 3
NCH = 2
ROWS = EXPERT * 2 * CAP
CR = ROWS // NCH
CO = EXPERT // NCH
PAIR = 2 * CAP


def local_copy(src, dst, sem):
    return pltpu.make_async_copy(src, dst, sem)


def remote(src, dst, ssem, rsem, **where):
    return pltpu.make_async_remote_copy(
        src_ref=src, dst_ref=dst, send_sem=ssem, recv_sem=rsem, device_id=where, device_id_type=MESH
    )


def wait_bytes(ref, sem):
    pltpu.make_async_copy(ref, ref, sem).wait()


def offset_of(o):
    dzi, dx = o // 4, o % 4
    return dx, ((dzi + 1) // 2) * (2 * (dzi % 2) - 1)


def dot_t(a, b):
    return lax.dot_general(a, b, (((1,), (1,)), ((), ())), preferred_element_type=f32)


def dot(a, b):
    return jnp.dot(a, b, preferred_element_type=f32)


def layer_kernel(
    clen, prow, plen, res, q, routes, rw, kv, pages, ow, gw, uw, dw,
    out,
    kvb, pgb, owb, gwb, uwb, dwb, resb,
    qall, psnd, prcv, own_m, own_top, own_tot, row_top, att,
    osnd, orcv, hid, selw, dsnd, xg, acc, act,
    xsnd, xrcv, part, ssnd, rrcv, fin, rsnd, ret, fsnd, fall,
    lsem, kvsem, qs, qr, ps, pr, os_, or_, ds_, dr, as_, ar, fs, fr,
    xs, xr, rs, rr, ts, tr, es, er,
):
    p = lax.axis_index("pool")
    e = lax.axis_index("expert")
    y, c = p // 2, p % 2
    ex, ez = e // 8, e % 8
    partner = y * 2 + (1 - c)
    head = p // 4
    scale = 1.0 / math.sqrt(128)

    barrier = pltpu.get_barrier_semaphore()

    def greet_pool(k, carry):
        pl.semaphore_signal(barrier, inc=1, device_id={"pool": (p + k) % POOL}, device_id_type=MESH)
        return carry

    def greet_expert(k, carry):
        pl.semaphore_signal(barrier, inc=1, device_id={"expert": (e + k) % EXPERT}, device_id_type=MESH)
        return carry

    lax.fori_loop(1, EXPERT, greet_expert, 0)
    lax.fori_loop(1, POOL, greet_pool, 0)

    for r in range(8):
        local_copy(kv.at[r, :, head], kvb.at[r], kvsem.at[r]).start()
    local_copy(pages.at[:, 0, :, 0], pgb.at[0], lsem.at[0]).start()
    local_copy(pages.at[:, 0, :, 1], pgb.at[1], lsem.at[1]).start()
    own_cols = pl.ds(pl.multiple_of(p * 512, 512), 512)
    local_copy(res.at[:, :, own_cols], resb, lsem.at[2]).start()
    local_copy(ow, owb, lsem.at[3]).start()
    local_copy(gw, gwb, lsem.at[4]).start()
    local_copy(uw, uwb, lsem.at[5]).start()
    local_copy(dw, dwb, lsem.at[6]).start()
    local_copy(q, qall.at[p], qr).start()

    lane = lax.broadcasted_iota(jnp.int32, (16, ROWS), 1).astype(f32)
    spot = jnp.floor((lane + 0.5) * (1.0 / PAIR))
    within = lane - spot * PAIR
    which = jnp.where(within >= CAP, 1.0, 0.0)
    slot = within - which * CAP
    dzi = jnp.floor((spot + 0.5) * 0.25)
    dx = spot - dzi * 4
    half = jnp.floor((dzi + 1.5) * 0.5)
    odd = dzi - 2.0 * jnp.floor((dzi + 0.5) * 0.5)
    dz = half * (2.0 * odd - 1.0)
    gx = ex.astype(f32) - dx
    gx = jnp.where(gx < 0, gx + 4, gx)
    gz = ez.astype(f32) - dz
    gz = jnp.where(gz < 0, gz + 8, jnp.where(gz >= 8, gz - 8, gz))
    expert_id = (gx * 8 + gz) * 2 + which
    names = routes[...].reshape(16, 8).astype(f32)
    strengths = rw[...].reshape(16, 8)
    chosen = jnp.zeros((16, ROWS), f32)
    strength = jnp.zeros((16, ROWS), f32)
    for k in range(8):
        hit = names[:, k : k + 1] == expert_id
        chosen = jnp.where(hit, 1.0, chosen)
        strength = jnp.where(hit, strengths[:, k : k + 1], strength)
    earlier = (
        lax.broadcasted_iota(jnp.int32, (16, 16), 1) < lax.broadcasted_iota(jnp.int32, (16, 16), 0)
    ).astype(f32).astype(bf16)
    before = dot(earlier, chosen.astype(bf16))
    taken = jnp.where(before == slot, chosen, 0.0)
    selw[0] = taken
    selw[1] = taken * strength

    def cache_row(r):
        keys = kvb.reshape(8, 1024, 128)[r]
        s = dot_t(q[r].reshape(8, 128), keys) * scale
        col = lax.broadcasted_iota(jnp.int32, (8, 1024), 1)
        step = lax.broadcasted_iota(jnp.int32, (8, 1024), 0) // 4
        seen = (col % 2 == 0) & (col <= 2 * (clen[r] + step))
        top = jnp.max(jnp.where(seen, s, very_low), axis=1, keepdims=True)
        w = jnp.where(seen, jnp.exp(s - top), 0.0)
        own_top[r] = jnp.broadcast_to(top, (8, 128))
        own_tot[r] = jnp.broadcast_to(jnp.sum(w, axis=1, keepdims=True), (8, 128))
        own_m[r] = dot(pltpu.roll(w, 1, 1).astype(bf16), keys)

    for r in range(4):
        local_copy(kv.at[r, :, head], kvb.at[r], kvsem.at[r]).wait()
    for r in range(4):
        cache_row(r)

    pl.semaphore_wait(barrier, EXPERT - 1 + POOL - 1)

    def send_query(k, carry):
        remote(q, qall.at[p], qs, qr, pool=(p + k) % POOL).start()
        return carry

    lax.fori_loop(1, POOL, send_query, 0)

    for r in range(4, 8):
        local_copy(kv.at[r, :, head], kvb.at[r], kvsem.at[r]).wait()
    for r in range(4, 8):
        cache_row(r)

    local_copy(pages.at[:, 0, :, 0], pgb.at[0], lsem.at[0]).wait()
    local_copy(pages.at[:, 0, :, 1], pgb.at[1], lsem.at[1]).wait()
    wait_bytes(qall, qr)
    lane128 = lax.broadcasted_iota(jnp.int32, (32, 128), 1)
    for s_ in range(4):
        row = prow[p * 4 + s_]
        filled = plen[p * 4 + s_]
        for g in range(2):
            keys = pgb.reshape(2, 4, 128, 128)[g, s_]
            asked = jnp.concatenate([qall[4 * g + i, row].reshape(8, 128) for i in range(4)], axis=0)
            s = dot_t(asked, keys) * scale
            seen = (lane128 % 2 == 0) & (lane128 < 2 * filled)
            top = jnp.max(jnp.where(seen, s, very_low), axis=1, keepdims=True)
            top = top.astype(bf16).astype(f32)
            w = jnp.where(seen, jnp.exp(s - top), 0.0)
            total = jnp.sum(w, axis=1, keepdims=True)
            mixed = dot(pltpu.roll(w, 1, 1).astype(bf16), keys).astype(bf16)
            high = total.astype(bf16).astype(f32)
            stats = jnp.where(lane128 < 32, top, jnp.where(lane128 < 64, high, total - high)).astype(bf16)
            for i in range(4):
                psnd[4 * g + i, 0, s_ * 8 : s_ * 8 + 8] = mixed[i * 8 : i * 8 + 8]
                psnd[4 * g + i, 1, s_ * 8 : s_ * 8 + 8] = stats[i * 8 : i * 8 + 8]

    local_copy(psnd.at[p], prcv.at[p], pr).start()

    def send_parts(k, carry):
        to = (p + k) % POOL
        remote(psnd.at[to], prcv.at[p], ps, pr, pool=to).start()
        return carry

    lax.fori_loop(1, POOL, send_parts, 0)
    local_copy(ow, owb, lsem.at[3]).wait()
    local_copy(res.at[:, :, own_cols], resb, lsem.at[2]).wait()
    wait_bytes(prcv, pr)

    tops = [own_top[r] for r in range(8)]
    match = []
    for n in range(32):
        st = prcv[n // 4, 1, (n % 4) * 8 : (n % 4) * 8 + 8].astype(f32)
        top = jnp.broadcast_to(st[:, 0:1], (8, 128))
        row = prow[n]
        flags = [jnp.where(row == r, 1.0, 0.0) for r in range(8)]
        match.append(flags)
        for r in range(8):
            tops[r] = jnp.maximum(tops[r], top + (flags[r] - 1.0) * 2e30)
    for r in range(8):
        row_top[r] = tops[r]
    nums, dens = [], []
    for r in range(8):
        factor = jnp.exp(own_top[r] - tops[r])
        nums.append(own_m[r] * factor)
        dens.append(own_tot[r] * factor)
    for n in range(32):
        st = prcv[n // 4, 1, (n % 4) * 8 : (n % 4) * 8 + 8].astype(f32)
        top = jnp.broadcast_to(st[:, 0:1], (8, 128))
        total = jnp.broadcast_to(st[:, 32:33] + st[:, 64:65], (8, 128))
        factor = jnp.exp(top - row_top[prow[n]])
        mixed = prcv[n // 4, 0, (n % 4) * 8 : (n % 4) * 8 + 8].astype(f32) * factor
        total = total * factor
        for r in range(8):
            nums[r] = nums[r] + mixed * match[n][r]
            dens[r] = dens[r] + total * match[n][r]
    for r in range(8):
        att[r * 8 : r * 8 + 8] = nums[r] / dens[r]
    attended = jnp.concatenate(
        [att[pl.ds(h, 16, stride=4), :].astype(bf16) for h in range(4)], axis=1
    )

    def project(k):
        to = (p + k) % POOL
        return to, dot(attended, owb[:, pl.ds(pl.multiple_of(to * 512, 512), 512)])

    for k in (4, 3, 5, 2, 6, 1, 7):
        to, value = project(k)
        osnd[k - 1] = value.astype(bf16)
        remote(osnd.at[k - 1], orcv.at[k - 1], os_.at[k - 1], or_.at[k - 1], pool=to).start()
    _, hidden = project(0)
    hidden = hidden + resb[...].reshape(16, 512).astype(f32)
    for k in range(1, 8):
        remote(osnd.at[k - 1], orcv.at[k - 1], os_.at[k - 1], or_.at[k - 1], pool=p).wait_recv()
        hidden = hidden + orcv[k - 1].astype(f32)
    hid[...] = hidden

    leaving = lax.dot_general(
        selw[0].astype(bf16), hidden.astype(bf16), (((0,), (0,)), ((), ())), preferred_element_type=f32
    ).astype(bf16)
    for b in range(4):
        dsnd[b] = leaving[:, b * 128 : (b + 1) * 128]

    def rows_of(o):
        return pl.ds(pl.multiple_of(o * PAIR, 2), PAIR)

    def chunk_rows(ch):
        return pl.ds(ch * CR, CR)

    local_copy(dsnd.at[:, pl.ds(0, PAIR), :], xg.at[p, :, pl.ds(0, PAIR), :], dr.at[0]).start()
    for ch in range(NCH):

        def send_rows(o, carry):
            dx_, dz_ = offset_of(o)
            to = ((ex - dx_ + 4) % 4) * 8 + (ez - dz_ + 8) % 8
            remote(
                dsnd.at[:, rows_of(o), :], xg.at[p, :, rows_of(o), :], ds_.at[ch], dr.at[ch], expert=to
            ).start()
            return carry

        lax.fori_loop(max(1, ch * CO), (ch + 1) * CO, send_rows, 0)

    def share(dy, core):
        return ((y + dy) % 4) * 2 + core

    def block_of(s, ch):
        return xg.at[s, :, chunk_rows(ch), :]

    def give(ch, dy):
        to = share(dy, c)
        return remote(block_of(p, ch), block_of(p, ch), as_.at[ch, dy], ar.at[ch, dy], pool=to)

    def pass_on(ch, dy):
        s = share(dy, c)
        return remote(block_of(s, ch), block_of(s, ch), fs.at[ch, dy], fr.at[ch, dy], pool=partner)

    def upward(ch, s, first=False):
        rows = jnp.concatenate([xg[s, b, chunk_rows(ch), :] for b in range(4)], axis=1)
        at = pl.ds(pl.multiple_of(s * 512, 512), 512)
        for j in range(2):
            w = jnp.concatenate([gwb[j, at, :], uwb[j, at, :]], axis=1)
            value = dot(rows, w)
            if first:
                acc[ch, j] = value
            else:
                acc[ch, j] += value

    for ch in range(NCH):
        wait_bytes(block_of(p, ch), dr.at[ch])
        for dy in (1, 3, 2):
            give(ch, dy).start()
        pass_on(ch, 0).start()
        if ch == 0:
            local_copy(gw, gwb, lsem.at[4]).wait()
            local_copy(uw, uwb, lsem.at[5]).wait()
        upward(ch, p, True)

    local_copy(dw, dwb, lsem.at[6]).wait()

    def experts(ch):
        pass_on(ch, 0).wait_recv()
        upward(ch, partner)
        for dy in (1, 3, 2):
            give(ch, (4 - dy) % 4).wait_recv()
            pass_on(ch, dy).start()
            upward(ch, share(dy, c))
        for dy in (1, 3, 2):
            pass_on(ch, dy).wait_recv()
            upward(ch, share(dy, 1 - c))
        row = lax.broadcasted_iota(jnp.int32, (CR, 128), 0).astype(f32)
        within = row - jnp.floor((row + 0.5) * (1.0 / PAIR)) * PAIR
        parts = []
        for j in range(2):
            gate, up = acc[ch, j, :, 0:128], acc[ch, j, :, 128:256]
            value = gate / (1.0 + jnp.exp(-gate)) * up
            mine = (within >= CAP) if j else (within < CAP)
            parts.append(jnp.where(mine, value, 0.0).astype(bf16))
        act[...] = jnp.concatenate(parts, axis=1)

    def down(s):
        at = pl.ds(pl.multiple_of(s * 512, 512), 512)
        return dot(act[...], dwb.reshape(256, 4096)[:, at])

    def across(ch, dy):
        return remote(xsnd.at[ch, dy], xrcv.at[ch, dy], xs.at[ch, dy], xr.at[ch, dy], pool=partner)

    def home(ch, dy):
        return remote(ssnd.at[ch, dy - 1], rrcv.at[ch, dy - 1], rs.at[ch, dy - 1], rr.at[ch, dy - 1], pool=share(dy, c))

    def outward(ch):
        for dy in (2, 1, 3, 0):
            value = down(share(dy, 1 - c)).astype(bf16)
            for b in range(4):
                xsnd[ch, dy, b] = value[:, b * 128 : (b + 1) * 128]
            across(ch, dy).start()
        for dy in (2, 1, 3, 0):
            part[dy] = down(share(dy, c))
        for dy in (2, 1, 3, 0):
            across(ch, dy).wait_recv()
            for b in range(4):
                value = part[dy, :, b * 128 : (b + 1) * 128] + xrcv[ch, dy, b].astype(f32)
                if dy:
                    ssnd[ch, dy - 1, b] = value.astype(bf16)
                else:
                    fin[b, chunk_rows(ch), :] = value
            if dy:
                home(ch, dy).start()

    def back(ch):
        for dy in (1, 3, 2):
            home(ch, dy).wait_recv()
        for b in range(4):
            value = fin[b, chunk_rows(ch), :]
            for dy in (1, 2, 3):
                value = value + rrcv[ch, dy - 1, b].astype(f32)
            rsnd[b, chunk_rows(ch), :] = value.astype(bf16)
        if ch == 0:
            local_copy(rsnd.at[:, pl.ds(0, PAIR), :], ret.at[:, pl.ds(0, PAIR), :], tr.at[0]).start()

        def send_rows(o, carry):
            dx_, dz_ = offset_of(o)
            to = ((ex + dx_) % 4) * 8 + (ez + dz_ + 8) % 8
            remote(rsnd.at[:, rows_of(o), :], ret.at[:, rows_of(o), :], ts.at[ch], tr.at[ch], expert=to).start()
            return carry

        lax.fori_loop(max(1, ch * CO), (ch + 1) * CO, send_rows, 0)

    experts(0)
    outward(0)
    for ch in range(1, NCH):
        experts(ch)
        outward(ch)
        back(ch - 1)
    back(NCH - 1)

    for ch in range(NCH):
        wait_bytes(ret.at[:, chunk_rows(ch), :], tr.at[ch])
    high = selw[1].astype(bf16)
    low = (selw[1] - high.astype(f32)).astype(bf16)
    returned = jnp.concatenate([ret[b] for b in range(4)], axis=1)
    summed = dot(jnp.concatenate([high, low], axis=0), returned)
    fsnd[...] = (hid[...] + (summed[0:16] + summed[16:32])).astype(bf16)
    local_copy(fsnd, fall.at[p], er).start()

    def send_result(k, carry):
        remote(fsnd, fall.at[p], es, er, pool=(p + k) % POOL).start()
        return carry

    lax.fori_loop(1, POOL, send_result, 0)
    wait_bytes(fall, er)
    for s in range(POOL):
        out[:, :, s * 512 : (s + 1) * 512] = fall[s].reshape(8, 2, 512)

    wait_bytes(qall.at[pl.ds(0, POOL - 1)], qs)
    wait_bytes(psnd.at[pl.ds(0, POOL - 1)], ps)
    wait_bytes(fall.at[pl.ds(0, POOL - 1)], es)
    for k in range(1, 8):
        remote(osnd.at[k - 1], orcv.at[k - 1], os_.at[k - 1], or_.at[k - 1], pool=p).wait_send()
    for ch in range(NCH):
        sent = pl.ds(0, CR - PAIR if ch == 0 else CR)
        wait_bytes(dsnd.at[:, sent, :], ds_.at[ch])
        wait_bytes(rsnd.at[:, sent, :], ts.at[ch])
        for dy in range(4):
            if dy:
                give(ch, dy).wait_send()
                home(ch, dy).wait_send()
            pass_on(ch, dy).wait_send()
            across(ch, dy).wait_send()


def per_device(
    residual, queries, kv_cache, kv_pages, cache_len, page_row, page_len, routes, route_weight,
    out_weight, gate_weight, up_weight, down_weight,
):
    smem = pl.BlockSpec(memory_space=pltpu.SMEM)
    vmem = pl.BlockSpec(memory_space=pltpu.VMEM)
    anywhere = pl.BlockSpec(memory_space=pl.ANY)
    dma = pltpu.SemaphoreType.DMA
    V = pltpu.VMEM
    return pl.pallas_call(
        layer_kernel,
        name="layer",
        out_shape=jax.ShapeDtypeStruct(residual.shape, bf16),
        in_specs=[smem] * 3 + [anywhere] + [vmem] * 3 + [anywhere] * 6,
        out_specs=vmem,
        scratch_shapes=[
            V((8, 512, 2, 128), bf16),
            V((2, 4, 64, 2, 128), bf16),
            V((512, 4096), bf16),
            V((2, 4096, 128), bf16),
            V((2, 4096, 128), bf16),
            V((2, 128, 4096), bf16),
            V((8, 2, 512), bf16),
            V((8, 8, 2, 4, 128), bf16),
            V((8, 2, 32, 128), bf16),
            V((8, 2, 32, 128), bf16),
            V((8, 8, 128), f32),
            V((8, 8, 128), f32),
            V((8, 8, 128), f32),
            V((8, 8, 128), f32),
            V((64, 128), f32),
            V((7, 16, 512), bf16),
            V((7, 16, 512), bf16),
            V((16, 512), f32),
            V((2, 16, ROWS), f32),
            V((4, ROWS, 128), bf16),
            V((8, 4, ROWS, 128), bf16),
            V((NCH, 2, CR, 256), f32),
            V((CR, 256), bf16),
            V((NCH, 4, 4, CR, 128), bf16),
            V((NCH, 4, 4, CR, 128), bf16),
            V((4, CR, 512), f32),
            V((NCH, 3, 4, CR, 128), bf16),
            V((NCH, 3, 4, CR, 128), bf16),
            V((4, ROWS, 128), f32),
            V((4, ROWS, 128), bf16),
            V((4, ROWS, 128), bf16),
            V((16, 512), bf16),
            V((8, 16, 512), bf16),
            dma((7,)), dma((8,)), dma(()), dma(()), dma(()), dma(()), dma((7,)), dma((7,)),
            dma((NCH,)), dma((NCH,)), dma((NCH, 4)), dma((NCH, 4)), dma((NCH, 4)), dma((NCH, 4)),
            dma((NCH, 4)), dma((NCH, 4)), dma((NCH, 3)), dma((NCH, 3)), dma((NCH,)), dma((NCH,)),
            dma(()), dma(()),
        ],
        compiler_params=pltpu.CompilerParams(
            collective_id=0, has_side_effects=True, vmem_limit_bytes=60 * 1024 * 1024
        ),
    )(
        cache_len, page_row.reshape(32), page_len.reshape(32), residual, queries, routes, route_weight,
        kv_cache, kv_pages, out_weight, gate_weight, up_weight, down_weight,
    )


def solution(mesh):
    return jax.shard_map(
        per_device,
        mesh=mesh,
        in_specs=(
            P("expert", None, None),
            P("expert", None, "pool", None),
            P("expert", None, None, None, None),
            P("pool", "expert", None, None, None, None),
            P("expert"),
            P(None, "expert"),
            P(None, "expert"),
            P("expert", None, None),
            P("expert", None, None),
            P("pool", None),
            P("expert", None, "pool"),
            P("expert", None, "pool"),
            P("expert", "pool", None),
        ),
        out_specs=P("expert", None, None),
        check_vma=False,
    )
```

```python
import functools
import math

import jax
import jax.numpy as jnp
from jax import lax
from jax.experimental import pallas as pl
from jax.experimental.pallas import tpu as pltpu
from jax.sharding import PartitionSpec as P

very_low = -1e30
MESH = pl.DeviceIdType.MESH
bf16, f32 = jnp.bfloat16, jnp.float32
POOL, EXPERT = 8, 32
CAP = 3
NCH = 4
ROT = 2
ROWS = EXPERT * 2 * CAP
CR = ROWS // NCH
CO = EXPERT // NCH
PAIR = 2 * CAP
SELF = (-ROT) % 8 * 4


def local_copy(src, dst, sem):
    return pltpu.make_async_copy(src, dst, sem)


def remote(src, dst, ssem, rsem, **where):
    return pltpu.make_async_remote_copy(
        src_ref=src, dst_ref=dst, send_sem=ssem, recv_sem=rsem, device_id=where, device_id_type=MESH
    )


def wait_bytes(ref, sem):
    pltpu.make_async_copy(ref, ref, sem).wait()


def offset_of(o):
    dzi, dx = (o // 4 + ROT) % 8, o % 4
    return dx, ((dzi + 1) // 2) * (2 * (dzi % 2) - 1)


def dot_t(a, b):
    return lax.dot_general(a, b, (((1,), (1,)), ((), ())), preferred_element_type=f32)


def dot(a, b):
    return jnp.dot(a, b, preferred_element_type=f32)


def layer_kernel(
    clen, prow, plen, res, q, routes, rw, kv, pages, ow, gw, uw, dw,
    out,
    kvb, pgb, owb, gwb, uwb, dwb, resb,
    qall, psnd, prcv, own_m, own_top, own_tot, row_top, att,
    osnd, orcv, hid, selw, picks, q8, dsnd, xg, acc, act,
    xsnd, xrcv, part, ssnd, rrcv, fin, rsnd, ret, fsnd, fall,
    lsem, kvsem, qs, qr, ps, pr, os_, or_, ds_, dr, as_, ar, fs, fr,
    xs, xr, rs, rr, ts, tr, es, er,
):
    p = lax.axis_index("pool")
    e = lax.axis_index("expert")
    y, c = p // 2, p % 2
    ex, ez = e // 8, e % 8
    partner = y * 2 + (1 - c)
    head = p // 4
    scale = 1.0 / math.sqrt(128)

    barrier = pltpu.get_barrier_semaphore()

    def greet_pool(k, carry):
        pl.semaphore_signal(barrier, inc=1, device_id={"pool": (p + k) % POOL}, device_id_type=MESH)
        return carry

    def greet_expert(k, carry):
        pl.semaphore_signal(barrier, inc=1, device_id={"expert": (e + k) % EXPERT}, device_id_type=MESH)
        return carry

    lax.fori_loop(1, EXPERT, greet_expert, 0)
    lax.fori_loop(1, POOL, greet_pool, 0)

    for r in range(8):
        local_copy(kv.at[r, :, head], kvb.at[r], kvsem.at[r]).start()
    local_copy(pages.at[:, 0, :, 0], pgb.at[0], lsem.at[0]).start()
    local_copy(pages.at[:, 0, :, 1], pgb.at[1], lsem.at[1]).start()
    own_cols = pl.ds(pl.multiple_of(p * 512, 512), 512)
    local_copy(res.at[:, :, own_cols], resb, lsem.at[2]).start()
    local_copy(ow, owb, lsem.at[3]).start()
    local_copy(gw, gwb, lsem.at[4]).start()
    local_copy(uw, uwb, lsem.at[5]).start()
    local_copy(dw, dwb, lsem.at[6]).start()

    lane = lax.broadcasted_iota(jnp.int32, (16, ROWS), 1).astype(f32)
    spot = jnp.floor((lane + 0.5) * (1.0 / PAIR))
    within = lane - spot * PAIR
    which = jnp.where(within >= CAP, 1.0, 0.0)
    slot = within - which * CAP
    dzi = jnp.floor((spot + 0.5) * 0.25)
    dx = spot - dzi * 4
    dzi = dzi + ROT
    dzi = jnp.where(dzi >= 8, dzi - 8, dzi)
    half = jnp.floor((dzi + 1.5) * 0.5)
    odd = dzi - 2.0 * jnp.floor((dzi + 0.5) * 0.5)
    dz = half * (2.0 * odd - 1.0)
    gx = ex.astype(f32) - dx
    gx = jnp.where(gx < 0, gx + 4, gx)
    gz = ez.astype(f32) - dz
    gz = jnp.where(gz < 0, gz + 8, jnp.where(gz >= 8, gz - 8, gz))
    expert_id = (gx * 8 + gz) * 2 + which
    names = routes[...].reshape(16, 8).astype(f32)
    strengths = rw[...].reshape(16, 8)
    chosen = jnp.zeros((16, ROWS), f32)
    strength = jnp.zeros((16, ROWS), f32)
    for k in range(8):
        hit = names[:, k : k + 1] == expert_id
        chosen = jnp.where(hit, 1.0, chosen)
        strength = jnp.where(hit, strengths[:, k : k + 1], strength)
    earlier = (
        lax.broadcasted_iota(jnp.int32, (16, 16), 1) < lax.broadcasted_iota(jnp.int32, (16, 16), 0)
    ).astype(f32).astype(bf16)
    before = dot(earlier, chosen.astype(bf16))
    taken = jnp.where(before == slot, chosen, 0.0)
    picks[...] = taken.T.astype(bf16)
    selw[...] = taken * strength
    q8[...] = q[...].reshape(8, 8, 128)

    def cache_row(r):
        keys = kvb.reshape(8, 1024, 128)[r]
        s = dot_t(q8[r], keys) * scale
        col = lax.broadcasted_iota(jnp.int32, (8, 1024), 1)
        step = lax.broadcasted_iota(jnp.int32, (8, 1024), 0) // 4
        seen = (col % 2 == 0) & (col <= 2 * (clen[r] + step))
        top = jnp.max(jnp.where(seen, s, very_low), axis=1, keepdims=True)
        w = jnp.where(seen, jnp.exp(s - top), 0.0)
        own_top[r] = jnp.broadcast_to(top, (8, 128))
        own_tot[r] = jnp.broadcast_to(jnp.sum(w, axis=1, keepdims=True), (8, 128))
        own_m[r] = dot(pltpu.roll(w, 1, 1).astype(bf16), keys)

    for r in range(4):
        local_copy(kv.at[r, :, head], kvb.at[r], kvsem.at[r]).wait()
    for r in range(4):
        cache_row(r)

    pl.semaphore_wait(barrier, EXPERT - 1 + POOL - 1)

    def send_query(k, carry):
        remote(q8, qall.at[p], qs, qr, pool=(p + k) % POOL).start()
        return carry

    lax.fori_loop(1, POOL, send_query, 0)
    local_copy(q8, qall.at[p], qr).start()

    for r in range(4, 8):
        local_copy(kv.at[r, :, head], kvb.at[r], kvsem.at[r]).wait()
    for r in range(4, 8):
        cache_row(r)

    local_copy(pages.at[:, 0, :, 0], pgb.at[0], lsem.at[0]).wait()
    local_copy(pages.at[:, 0, :, 1], pgb.at[1], lsem.at[1]).wait()
    wait_bytes(qall, qr)
    scores = []
    for s_ in range(4):
        row = prow[p * 4 + s_]
        for g in range(2):
            asked = jnp.concatenate([qall[4 * g + i, row] for i in range(4)], axis=0)
            scores.append(dot_t(asked, pgb.reshape(2, 4, 128, 128)[g, s_]))
    scores = jnp.concatenate(scores, axis=0) * scale
    lane128 = lax.broadcasted_iota(jnp.int32, (256, 128), 1)
    limit = jnp.concatenate([jnp.full((64, 128), 2 * plen[p * 4 + s_], jnp.int32) for s_ in range(4)], axis=0)
    seen = (lane128 % 2 == 0) & (lane128 < limit)
    top = jnp.max(jnp.where(seen, scores, very_low), axis=1, keepdims=True)
    top = top.astype(bf16).astype(f32)
    w = jnp.where(seen, jnp.exp(scores - top), 0.0)
    total = jnp.sum(w, axis=1, keepdims=True)
    w = pltpu.roll(w, 1, 1).astype(bf16)
    high = total.astype(bf16).astype(f32)
    stats = jnp.where(lane128 < 32, top, jnp.where(lane128 < 64, high, total - high))
    for s_ in range(4):
        for g in range(2):
            at = (s_ * 2 + g) * 32
            mixed = dot(w[at : at + 32], pgb.reshape(2, 4, 128, 128)[g, s_])
            for i in range(4):
                psnd[4 * g + i, 0, s_ * 8 : s_ * 8 + 8] = mixed[i * 8 : i * 8 + 8].astype(bf16)
                psnd[4 * g + i, 1, s_ * 8 : s_ * 8 + 8] = stats[at + i * 8 : at + i * 8 + 8].astype(bf16)

    local_copy(psnd.at[p], prcv.at[p], pr).start()

    def send_parts(k, carry):
        to = (p + k) % POOL
        remote(psnd.at[to], prcv.at[p], ps, pr, pool=to).start()
        return carry

    lax.fori_loop(1, POOL, send_parts, 0)
    local_copy(ow, owb, lsem.at[3]).wait()
    local_copy(res.at[:, :, own_cols], resb, lsem.at[2]).wait()
    wait_bytes(prcv, pr)

    tops = [own_top[r] for r in range(8)]
    match = []
    for n in range(32):
        st = prcv[n // 4, 1, (n % 4) * 8 : (n % 4) * 8 + 8].astype(f32)
        top = jnp.broadcast_to(st[:, 0:1], (8, 128))
        row = prow[n]
        flags = [jnp.where(row == r, 1.0, 0.0) for r in range(8)]
        match.append(flags)
        for r in range(8):
            tops[r] = jnp.maximum(tops[r], top + (flags[r] - 1.0) * 2e30)
    for r in range(8):
        row_top[r] = tops[r]
    nums, dens = [], []
    for r in range(8):
        factor = jnp.exp(own_top[r] - tops[r])
        nums.append(own_m[r] * factor)
        dens.append(own_tot[r] * factor)
    for n in range(32):
        st = prcv[n // 4, 1, (n % 4) * 8 : (n % 4) * 8 + 8].astype(f32)
        top = jnp.broadcast_to(st[:, 0:1], (8, 128))
        total = jnp.broadcast_to(st[:, 32:33] + st[:, 64:65], (8, 128))
        factor = jnp.exp(top - row_top[prow[n]])
        mixed = prcv[n // 4, 0, (n % 4) * 8 : (n % 4) * 8 + 8].astype(f32) * factor
        total = total * factor
        for r in range(8):
            nums[r] = nums[r] + mixed * match[n][r]
            dens[r] = dens[r] + total * match[n][r]
    for r in range(8):
        att[r * 8 : r * 8 + 8] = nums[r] / dens[r]
    attended = jnp.concatenate(
        [att[pl.ds(h, 16, stride=4), :].astype(bf16) for h in range(4)], axis=1
    )

    def project(k):
        to = (p + k) % POOL
        return to, dot(attended, owb[:, pl.ds(pl.multiple_of(to * 512, 512), 512)])

    for k in (4, 3, 5, 2, 6, 1, 7):
        to, value = project(k)
        osnd[k - 1] = value.astype(bf16)
        remote(osnd.at[k - 1], orcv.at[k - 1], os_.at[k - 1], or_.at[k - 1], pool=to).start()
    _, hidden = project(0)
    hidden = hidden + resb[...].reshape(16, 512).astype(f32)
    for k in range(1, 8):
        remote(osnd.at[k - 1], orcv.at[k - 1], os_.at[k - 1], or_.at[k - 1], pool=p).wait_recv()
        hidden = hidden + orcv[k - 1].astype(f32)
    hid[...] = hidden

    def rows_of(o):
        return pl.ds(pl.multiple_of(o * PAIR, 2), PAIR)

    def chunk_rows(ch):
        return pl.ds(ch * CR, CR)

    def each_offset(ch, body):
        first, last = ch * CO, (ch + 1) * CO
        if first <= SELF < last:
            lax.fori_loop(first, SELF, body, 0)
            lax.fori_loop(SELF + 1, last, body, 0)
        else:
            lax.fori_loop(first, last, body, 0)

    def stays(src, dst, sems):
        rows = pl.ds(SELF * PAIR, PAIR)
        local_copy(src.at[:, rows, :], dst.at[:, rows, :], sems.at[SELF // CO]).start()

    low_hidden = hidden.astype(bf16)
    for ch in range(NCH):
        leaving = dot(picks[chunk_rows(ch), :], low_hidden).astype(bf16)
        for b in range(4):
            dsnd[b, chunk_rows(ch), :] = leaving[:, b * 128 : (b + 1) * 128]

        def send_rows(o, carry, ch=ch):
            dx_, dz_ = offset_of(o)
            to = ((ex - dx_ + 4) % 4) * 8 + (ez - dz_ + 8) % 8
            remote(
                dsnd.at[:, rows_of(o), :], xg.at[p, :, rows_of(o), :], ds_.at[ch], dr.at[ch], expert=to
            ).start()
            return carry

        each_offset(ch, send_rows)
        if ch == SELF // CO:
            stays(dsnd, xg.at[p], dr)

    def share(dy, core):
        return ((y + dy) % 4) * 2 + core

    def block_of(s, ch):
        return xg.at[s, :, chunk_rows(ch), :]

    def give(ch, dy):
        to = share(dy, c)
        return remote(block_of(p, ch), block_of(p, ch), as_.at[ch, dy], ar.at[ch, dy], pool=to)

    def pass_on(ch, dy):
        s = share(dy, c)
        return remote(block_of(s, ch), block_of(s, ch), fs.at[ch, dy], fr.at[ch, dy], pool=partner)

    def upward(ch, s, first=False):
        rows = jnp.concatenate([xg[s, b, chunk_rows(ch), :] for b in range(4)], axis=1)
        at = pl.ds(pl.multiple_of(s * 512, 512), 512)
        for j in range(2):
            w = jnp.concatenate([gwb[j, at, :], uwb[j, at, :]], axis=1)
            value = dot(rows, w)
            if first:
                acc[ch, j] = value
            else:
                acc[ch, j] += value

    for ch in range(NCH):
        wait_bytes(block_of(p, ch), dr.at[ch])
        for dy in (1, 3, 2):
            give(ch, dy).start()
        pass_on(ch, 0).start()
        if ch == 0:
            local_copy(gw, gwb, lsem.at[4]).wait()
            local_copy(uw, uwb, lsem.at[5]).wait()
        upward(ch, p, True)

    local_copy(dw, dwb, lsem.at[6]).wait()

    def relay(ch, then=None):
        for dy in (1, 3, 2):
            give(ch, (4 - dy) % 4).wait_recv()
            pass_on(ch, dy).start()
            if then is not None:
                then(dy)

    def experts(ch):
        pass_on(ch, 0).wait_recv()
        upward(ch, partner)
        if ch == 0:
            relay(ch, lambda dy: upward(ch, share(dy, c)))
        else:
            for dy in (1, 3, 2):
                upward(ch, share(dy, c))
        for dy in (1, 3, 2):
            pass_on(ch, dy).wait_recv()
            upward(ch, share(dy, 1 - c))
        row = lax.broadcasted_iota(jnp.int32, (CR, 128), 0).astype(f32)
        within = row - jnp.floor((row + 0.5) * (1.0 / PAIR)) * PAIR
        parts = []
        for j in range(2):
            gate, up = acc[ch, j, :, 0:128], acc[ch, j, :, 128:256]
            value = gate / (1.0 + jnp.exp(-gate)) * up
            mine = (within >= CAP) if j else (within < CAP)
            parts.append(jnp.where(mine, value, 0.0).astype(bf16))
        act[...] = jnp.concatenate(parts, axis=1)

    def down(s):
        at = pl.ds(pl.multiple_of(s * 512, 512), 512)
        return dot(act[...], dwb.reshape(256, 4096)[:, at])

    def across(ch, dy):
        return remote(xsnd.at[ch, dy], xrcv.at[ch, dy], xs.at[ch, dy], xr.at[ch, dy], pool=partner)

    def home(ch, dy):
        return remote(ssnd.at[ch, dy - 1], rrcv.at[ch, dy - 1], rs.at[ch, dy - 1], rr.at[ch, dy - 1], pool=share(dy, c))

    def lend(ch):
        for dy in (2, 1, 3, 0):
            value = down(share(dy, 1 - c)).astype(bf16)
            for b in range(4):
                xsnd[ch, dy, b] = value[:, b * 128 : (b + 1) * 128]
            across(ch, dy).start()

    def keep():
        for dy in (2, 1, 3, 0):
            part[dy] = down(share(dy, c))

    def join(ch):
        for dy in (2, 1, 3, 0):
            across(ch, dy).wait_recv()
            for b in range(4):
                value = part[dy, :, b * 128 : (b + 1) * 128] + xrcv[ch, dy, b].astype(f32)
                if dy:
                    ssnd[ch, dy - 1, b] = value.astype(bf16)
                else:
                    fin[b, chunk_rows(ch), :] = value
            if dy:
                home(ch, dy).start()

    def back(ch):
        for dy in (1, 3, 2):
            home(ch, dy).wait_recv()
        for b in range(4):
            value = fin[b, chunk_rows(ch), :]
            for dy in (1, 2, 3):
                value = value + rrcv[ch, dy - 1, b].astype(f32)
            rsnd[b, chunk_rows(ch), :] = value.astype(bf16)

        def send_rows(o, carry):
            dx_, dz_ = offset_of(o)
            to = ((ex + dx_) % 4) * 8 + (ez + dz_ + 8) % 8
            remote(rsnd.at[:, rows_of(o), :], ret.at[:, rows_of(o), :], ts.at[ch], tr.at[ch], expert=to).start()
            return carry

        each_offset(ch, send_rows)
        if ch == SELF // CO:
            stays(rsnd, ret, tr)

    for ch in range(NCH):
        experts(ch)
        lend(ch)
        if ch + 1 < NCH:
            relay(ch + 1)
        if ch:
            join(ch - 1)
        keep()
        if ch >= 3:
            back(ch - 3)
    join(NCH - 1)
    for ch in range(max(0, NCH - 3), NCH):
        back(ch)

    for ch in range(NCH):
        wait_bytes(ret.at[:, chunk_rows(ch), :], tr.at[ch])
    high = selw[...].astype(bf16)
    low = (selw[...] - high.astype(f32)).astype(bf16)
    returned = jnp.concatenate([ret[b] for b in range(4)], axis=1)
    summed = dot(jnp.concatenate([high, low], axis=0), returned)
    fsnd[...] = (hid[...] + (summed[0:16] + summed[16:32])).astype(bf16)
    local_copy(fsnd, fall.at[p], er).start()

    def send_result(k, carry):
        remote(fsnd, fall.at[p], es, er, pool=(p + k) % POOL).start()
        return carry

    lax.fori_loop(1, POOL, send_result, 0)
    wait_bytes(fall, er)
    for s in range(POOL):
        out[:, s * 512 : (s + 1) * 512] = fall[s]

    wait_bytes(qall.at[pl.ds(0, POOL - 1)], qs)
    wait_bytes(psnd.at[pl.ds(0, POOL - 1)], ps)
    wait_bytes(fall.at[pl.ds(0, POOL - 1)], es)
    for k in range(1, 8):
        remote(osnd.at[k - 1], orcv.at[k - 1], os_.at[k - 1], or_.at[k - 1], pool=p).wait_send()
    for ch in range(NCH):
        sent = pl.ds(0, CR - PAIR if ch == SELF // CO else CR)
        wait_bytes(dsnd.at[:, sent, :], ds_.at[ch])
        wait_bytes(rsnd.at[:, sent, :], ts.at[ch])
        for dy in range(4):
            if dy:
                give(ch, dy).wait_send()
                home(ch, dy).wait_send()
            pass_on(ch, dy).wait_send()
            across(ch, dy).wait_send()


def per_device(
    residual, queries, kv_cache, kv_pages, cache_len, page_row, page_len, routes, route_weight,
    out_weight, gate_weight, up_weight, down_weight,
):
    smem = pl.BlockSpec(memory_space=pltpu.SMEM)
    vmem = pl.BlockSpec(memory_space=pltpu.VMEM)
    anywhere = pl.BlockSpec(memory_space=pl.ANY)
    dma = pltpu.SemaphoreType.DMA
    V = pltpu.VMEM
    gathered = pl.pallas_call(
        layer_kernel,
        name="layer",
        out_shape=jax.ShapeDtypeStruct((16, 4096), bf16),
        in_specs=[smem] * 3 + [anywhere] + [vmem] * 3 + [anywhere] * 6,
        out_specs=vmem,
        scratch_shapes=[
            V((8, 512, 2, 128), bf16),
            V((2, 4, 64, 2, 128), bf16),
            V((512, 4096), bf16),
            V((2, 4096, 128), bf16),
            V((2, 4096, 128), bf16),
            V((2, 128, 4096), bf16),
            V((8, 2, 512), bf16),
            V((8, 8, 8, 128), bf16),
            V((8, 2, 32, 128), bf16),
            V((8, 2, 32, 128), bf16),
            V((8, 8, 128), f32),
            V((8, 8, 128), f32),
            V((8, 8, 128), f32),
            V((8, 8, 128), f32),
            V((64, 128), f32),
            V((7, 16, 512), bf16),
            V((7, 16, 512), bf16),
            V((16, 512), f32),
            V((16, ROWS), f32),
            V((ROWS, 16), bf16),
            V((8, 8, 128), bf16),
            V((4, ROWS, 128), bf16),
            V((8, 4, ROWS, 128), bf16),
            V((NCH, 2, CR, 256), f32),
            V((CR, 256), bf16),
            V((NCH, 4, 4, CR, 128), bf16),
            V((NCH, 4, 4, CR, 128), bf16),
            V((4, CR, 512), f32),
            V((NCH, 3, 4, CR, 128), bf16),
            V((NCH, 3, 4, CR, 128), bf16),
            V((4, ROWS, 128), f32),
            V((4, ROWS, 128), bf16),
            V((4, ROWS, 128), bf16),
            V((16, 512), bf16),
            V((8, 16, 512), bf16),
            dma((7,)), dma((8,)), dma(()), dma(()), dma(()), dma(()), dma((7,)), dma((7,)),
            dma((NCH,)), dma((NCH,)), dma((NCH, 4)), dma((NCH, 4)), dma((NCH, 4)), dma((NCH, 4)),
            dma((NCH, 4)), dma((NCH, 4)), dma((NCH, 3)), dma((NCH, 3)), dma((NCH,)), dma((NCH,)),
            dma(()), dma(()),
        ],
        compiler_params=pltpu.CompilerParams(
            collective_id=0, has_side_effects=True, vmem_limit_bytes=60 * 1024 * 1024
        ),
    )(
        cache_len, page_row.reshape(32), page_len.reshape(32), residual, queries, routes, route_weight,
        kv_cache, kv_pages, out_weight, gate_weight, up_weight, down_weight,
    )
    return gathered.reshape(residual.shape)


def solution(mesh):
    return jax.shard_map(
        per_device,
        mesh=mesh,
        in_specs=(
            P("expert", None, None),
            P("expert", None, "pool", None),
            P("expert", None, None, None, None),
            P("pool", "expert", None, None, None, None),
            P("expert"),
            P(None, "expert"),
            P(None, "expert"),
            P("expert", None, None),
            P("expert", None, None),
            P("pool", None),
            P("expert", None, "pool"),
            P("expert", None, "pool"),
            P("expert", "pool", None),
        ),
        out_specs=P("expert", None, None),
        check_vma=False,
    )
```

```python
import functools
import math

import jax
import jax.numpy as jnp
from jax import lax
from jax.experimental import pallas as pl
from jax.experimental.pallas import tpu as pltpu
from jax.sharding import PartitionSpec as P

very_low = -1e30
MESH = pl.DeviceIdType.MESH
bf16, f32 = jnp.bfloat16, jnp.float32
POOL, EXPERT = 8, 32
CAP = 3
NCH = 4
ROT = 2
FAR_IN = (1, 2, 3)
FAR_OUT = (0, 1, 2)
ROWS = EXPERT * 2 * CAP
CR = ROWS // NCH
CO = EXPERT // NCH
PAIR = 2 * CAP
SELF = (-ROT) % 8 * 4


def local_copy(src, dst, sem):
    return pltpu.make_async_copy(src, dst, sem)


def remote(src, dst, ssem, rsem, **where):
    return pltpu.make_async_remote_copy(
        src_ref=src, dst_ref=dst, send_sem=ssem, recv_sem=rsem, device_id=where, device_id_type=MESH
    )


def wait_bytes(ref, sem):
    pltpu.make_async_copy(ref, ref, sem).wait()


def offset_of(o):
    dzi, dx = (o // 4 + ROT) % 8, o % 4
    return dx, ((dzi + 1) // 2) * (2 * (dzi % 2) - 1)


def dot_t(a, b):
    return lax.dot_general(a, b, (((1,), (1,)), ((), ())), preferred_element_type=f32)


def dot(a, b):
    return jnp.dot(a, b, preferred_element_type=f32)


def layer_kernel(
    clen, prow, plen, res, q, routes, rw, kv, pages, ow, gw, uw, dw,
    out,
    kvb, pgb, owb, gwb, uwb, dwb, resb,
    qall, psnd, prcv, own_m, own_top, own_tot, row_top, att,
    osnd, orcv, hid, selw, picks, q8, dsnd, xg, acc, act,
    xsnd, xrcv, part, ssnd, rrcv, fin, rsnd, ret, fsnd, fall,
    hsnd, hfar, dsnd2, rsnd2, ret2, wsnd, wrcv,
    lsem, kvsem, qs, qr, ps, pr, os_, or_, ds_, dr, as_, ar, fs, fr,
    xs, xr, rs, rr, ts, tr, es, er, gs, gr, d2s, d2r, t2s, t2r, ws, wr,
):
    p = lax.axis_index("pool")
    e = lax.axis_index("expert")
    y, c = p // 2, p % 2
    ex, ez = e // 8, e % 8
    partner = y * 2 + (1 - c)
    head = p // 4
    scale = 1.0 / math.sqrt(128)

    barrier = pltpu.get_barrier_semaphore()

    def greet_pool(k, carry):
        pl.semaphore_signal(barrier, inc=1, device_id={"pool": (p + k) % POOL}, device_id_type=MESH)
        return carry

    def greet_expert(k, carry):
        pl.semaphore_signal(barrier, inc=1, device_id={"expert": (e + k) % EXPERT}, device_id_type=MESH)
        return carry

    lax.fori_loop(1, EXPERT, greet_expert, 0)
    lax.fori_loop(1, POOL, greet_pool, 0)

    for r in range(8):
        local_copy(kv.at[r, :, head], kvb.at[r], kvsem.at[r]).start()
    local_copy(pages.at[:, 0, :, 0], pgb.at[0], lsem.at[0]).start()
    local_copy(pages.at[:, 0, :, 1], pgb.at[1], lsem.at[1]).start()
    own_cols = pl.ds(pl.multiple_of(p * 512, 512), 512)
    local_copy(res.at[:, :, own_cols], resb, lsem.at[2]).start()
    local_copy(ow, owb, lsem.at[3]).start()
    local_copy(gw, gwb, lsem.at[4]).start()
    local_copy(uw, uwb, lsem.at[5]).start()
    local_copy(dw, dwb, lsem.at[6]).start()

    lane = lax.broadcasted_iota(jnp.int32, (16, ROWS), 1).astype(f32)
    spot = jnp.floor((lane + 0.5) * (1.0 / PAIR))
    within = lane - spot * PAIR
    which = jnp.where(within >= CAP, 1.0, 0.0)
    slot = within - which * CAP
    dzi = jnp.floor((spot + 0.5) * 0.25)
    dx = spot - dzi * 4
    dzi = dzi + ROT
    dzi = jnp.where(dzi >= 8, dzi - 8, dzi)
    half = jnp.floor((dzi + 1.5) * 0.5)
    odd = dzi - 2.0 * jnp.floor((dzi + 0.5) * 0.5)
    dz = half * (2.0 * odd - 1.0)
    gx = ex.astype(f32) - dx
    gx = jnp.where(gx < 0, gx + 4, gx)
    gz = ez.astype(f32) - dz
    gz = jnp.where(gz < 0, gz + 8, jnp.where(gz >= 8, gz - 8, gz))
    expert_id = (gx * 8 + gz) * 2 + which
    names = routes[...].reshape(16, 8).astype(f32)
    strengths = rw[...].reshape(16, 8)
    chosen = jnp.zeros((16, ROWS), f32)
    strength = jnp.zeros((16, ROWS), f32)
    for k in range(8):
        hit = names[:, k : k + 1] == expert_id
        chosen = jnp.where(hit, 1.0, chosen)
        strength = jnp.where(hit, strengths[:, k : k + 1], strength)
    earlier = (
        lax.broadcasted_iota(jnp.int32, (16, 16), 1) < lax.broadcasted_iota(jnp.int32, (16, 16), 0)
    ).astype(f32).astype(bf16)
    before = dot(earlier, chosen.astype(bf16))
    taken = jnp.where(before == slot, chosen, 0.0)
    picks[...] = taken.T.astype(bf16)
    selw[...] = taken * strength
    q8[...] = q[...].reshape(8, 8, 128)

    def cache_row(r):
        keys = kvb.reshape(8, 1024, 128)[r]
        s = dot_t(q8[r], keys) * scale
        col = lax.broadcasted_iota(jnp.int32, (8, 1024), 1)
        step = lax.broadcasted_iota(jnp.int32, (8, 1024), 0) // 4
        seen = (col % 2 == 0) & (col <= 2 * (clen[r] + step))
        top = jnp.max(jnp.where(seen, s, very_low), axis=1, keepdims=True)
        w = jnp.where(seen, jnp.exp(s - top), 0.0)
        own_top[r] = jnp.broadcast_to(top, (8, 128))
        own_tot[r] = jnp.broadcast_to(jnp.sum(w, axis=1, keepdims=True), (8, 128))
        own_m[r] = dot(pltpu.roll(w, 1, 1).astype(bf16), keys)

    for r in range(4):
        local_copy(kv.at[r, :, head], kvb.at[r], kvsem.at[r]).wait()
    for r in range(4):
        cache_row(r)

    pl.semaphore_wait(barrier, EXPERT - 1 + POOL - 1)

    def send_query(k, carry):
        remote(q8, qall.at[p], qs, qr, pool=(p + k) % POOL).start()
        return carry

    lax.fori_loop(1, POOL, send_query, 0)
    local_copy(q8, qall.at[p], qr).start()

    for r in range(4, 8):
        local_copy(kv.at[r, :, head], kvb.at[r], kvsem.at[r]).wait()
    for r in range(4, 8):
        cache_row(r)

    local_copy(pages.at[:, 0, :, 0], pgb.at[0], lsem.at[0]).wait()
    local_copy(pages.at[:, 0, :, 1], pgb.at[1], lsem.at[1]).wait()
    wait_bytes(qall, qr)
    scores = []
    for s_ in range(4):
        row = prow[p * 4 + s_]
        for g in range(2):
            asked = jnp.concatenate([qall[4 * g + i, row] for i in range(4)], axis=0)
            scores.append(dot_t(asked, pgb.reshape(2, 4, 128, 128)[g, s_]))
    scores = jnp.concatenate(scores, axis=0) * scale
    lane128 = lax.broadcasted_iota(jnp.int32, (256, 128), 1)
    limit = jnp.concatenate([jnp.full((64, 128), 2 * plen[p * 4 + s_], jnp.int32) for s_ in range(4)], axis=0)
    seen = (lane128 % 2 == 0) & (lane128 < limit)
    top = jnp.max(jnp.where(seen, scores, very_low), axis=1, keepdims=True)
    top = top.astype(bf16).astype(f32)
    w = jnp.where(seen, jnp.exp(scores - top), 0.0)
    total = jnp.sum(w, axis=1, keepdims=True)
    w = pltpu.roll(w, 1, 1).astype(bf16)
    high = total.astype(bf16).astype(f32)
    stats = jnp.where(lane128 < 32, top, jnp.where(lane128 < 64, high, total - high))
    for s_ in range(4):
        for g in range(2):
            at = (s_ * 2 + g) * 32
            mixed = dot(w[at : at + 32], pgb.reshape(2, 4, 128, 128)[g, s_])
            for i in range(4):
                psnd[4 * g + i, 0, s_ * 8 : s_ * 8 + 8] = mixed[i * 8 : i * 8 + 8].astype(bf16)
                psnd[4 * g + i, 1, s_ * 8 : s_ * 8 + 8] = stats[at + i * 8 : at + i * 8 + 8].astype(bf16)

    local_copy(psnd.at[p], prcv.at[p], pr).start()

    def send_parts(k, carry):
        to = (p + k) % POOL
        remote(psnd.at[to], prcv.at[p], ps, pr, pool=to).start()
        return carry

    lax.fori_loop(1, POOL, send_parts, 0)
    local_copy(ow, owb, lsem.at[3]).wait()
    local_copy(res.at[:, :, own_cols], resb, lsem.at[2]).wait()
    wait_bytes(prcv, pr)

    tops = [own_top[r] for r in range(8)]
    match = []
    for n in range(32):
        st = prcv[n // 4, 1, (n % 4) * 8 : (n % 4) * 8 + 8].astype(f32)
        top = jnp.broadcast_to(st[:, 0:1], (8, 128))
        row = prow[n]
        flags = [jnp.where(row == r, 1.0, 0.0) for r in range(8)]
        match.append(flags)
        for r in range(8):
            tops[r] = jnp.maximum(tops[r], top + (flags[r] - 1.0) * 2e30)
    for r in range(8):
        row_top[r] = tops[r]
    nums, dens = [], []
    for r in range(8):
        factor = jnp.exp(own_top[r] - tops[r])
        nums.append(own_m[r] * factor)
        dens.append(own_tot[r] * factor)
    for n in range(32):
        st = prcv[n // 4, 1, (n % 4) * 8 : (n % 4) * 8 + 8].astype(f32)
        top = jnp.broadcast_to(st[:, 0:1], (8, 128))
        total = jnp.broadcast_to(st[:, 32:33] + st[:, 64:65], (8, 128))
        factor = jnp.exp(top - row_top[prow[n]])
        mixed = prcv[n // 4, 0, (n % 4) * 8 : (n % 4) * 8 + 8].astype(f32) * factor
        total = total * factor
        for r in range(8):
            nums[r] = nums[r] + mixed * match[n][r]
            dens[r] = dens[r] + total * match[n][r]
    for r in range(8):
        att[r * 8 : r * 8 + 8] = nums[r] / dens[r]
    attended = jnp.concatenate(
        [att[pl.ds(h, 16, stride=4), :].astype(bf16) for h in range(4)], axis=1
    )

    def project(k):
        to = (p + k) % POOL
        return to, dot(attended, owb[:, pl.ds(pl.multiple_of(to * 512, 512), 512)])

    for k in (4, 3, 5, 2, 6, 1, 7):
        to, value = project(k)
        osnd[k - 1] = value.astype(bf16)
        remote(osnd.at[k - 1], orcv.at[k - 1], os_.at[k - 1], or_.at[k - 1], pool=to).start()
    _, hidden = project(0)
    hidden = hidden + resb[...].reshape(16, 512).astype(f32)
    for k in range(1, 8):
        remote(osnd.at[k - 1], orcv.at[k - 1], os_.at[k - 1], or_.at[k - 1], pool=p).wait_recv()
        hidden = hidden + orcv[k - 1].astype(f32)
    hid[...] = hidden

    def rows_of(o):
        return pl.ds(pl.multiple_of(o * PAIR, 2), PAIR)

    def chunk_rows(ch):
        return pl.ds(ch * CR, CR)

    def each_offset(ch, body):
        first, last = ch * CO, (ch + 1) * CO
        if first <= SELF < last:
            lax.fori_loop(first, SELF, body, 0)
            lax.fori_loop(SELF + 1, last, body, 0)
        else:
            lax.fori_loop(first, last, body, 0)

    def stays(src, dst, sems):
        rows = pl.ds(SELF * PAIR, PAIR)
        local_copy(src.at[:, rows, :], dst.at[:, rows, :], sems.at[SELF // CO]).start()

    low_hidden = hidden.astype(bf16)
    across_ring = ((y + 2) % 4) * 2 + c
    hsnd[...] = low_hidden
    swap = remote(hsnd, hfar, gs, gr, pool=across_ring)
    swap.start()
    def depart(ch, columns, held, place, ssem, rsem):
        leaving = dot(picks[chunk_rows(ch), :], columns).astype(bf16)
        for b in range(4):
            held[b, chunk_rows(ch), :] = leaving[:, b * 128 : (b + 1) * 128]

        def send_rows(o, carry):
            dx_, dz_ = offset_of(o)
            to = ((ex - dx_ + 4) % 4) * 8 + (ez - dz_ + 8) % 8
            remote(
                held.at[:, rows_of(o), :], xg.at[place, :, rows_of(o), :], ssem.at[ch], rsem.at[ch], expert=to
            ).start()
            return carry

        each_offset(ch, send_rows)
        if ch == SELF // CO:
            stays(held, xg.at[place], rsem)

    for ch in range(NCH):
        depart(ch, low_hidden, dsnd, p, ds_, dr)
    swap.wait_recv()
    for ch in FAR_IN:
        depart(ch, hfar[...], dsnd2, across_ring, d2s, d2r)

    def share(dy, core):
        return ((y + dy) % 4) * 2 + core

    def block_of(s, ch):
        return xg.at[s, :, chunk_rows(ch), :]

    def give(ch, dy):
        to = share(dy, c)
        return remote(block_of(p, ch), block_of(p, ch), as_.at[ch, dy], ar.at[ch, dy], pool=to)

    def pass_on(ch, dy):
        s = share(dy, c)
        return remote(block_of(s, ch), block_of(s, ch), fs.at[ch, dy], fr.at[ch, dy], pool=partner)

    def upward(ch, s, first=False):
        rows = jnp.concatenate([xg[s, b, chunk_rows(ch), :] for b in range(4)], axis=1)
        at = pl.ds(pl.multiple_of(s * 512, 512), 512)
        for j in range(2):
            w = jnp.concatenate([gwb[j, at, :], uwb[j, at, :]], axis=1)
            value = dot(rows, w)
            if first:
                acc[ch, j] = value
            else:
                acc[ch, j] += value

    for ch in range(NCH):
        wait_bytes(block_of(p, ch), dr.at[ch])
        for dy in (1, 3) if ch in FAR_IN else (1, 3, 2):
            give(ch, dy).start()
        pass_on(ch, 0).start()
        if ch == 0:
            local_copy(gw, gwb, lsem.at[4]).wait()
            local_copy(uw, uwb, lsem.at[5]).wait()
        upward(ch, p, True)

    local_copy(dw, dwb, lsem.at[6]).wait()

    def relay(ch, then=None):
        for dy in (1, 3, 2):
            if dy == 2 and ch in FAR_IN:
                wait_bytes(block_of(across_ring, ch), d2r.at[ch])
            else:
                give(ch, (4 - dy) % 4).wait_recv()
            pass_on(ch, dy).start()
            if then is not None:
                then(dy)

    def experts(ch):
        pass_on(ch, 0).wait_recv()
        upward(ch, partner)
        if ch == 0:
            relay(ch, lambda dy: upward(ch, share(dy, c)))
        else:
            for dy in (1, 3, 2):
                upward(ch, share(dy, c))
        for dy in (1, 3, 2):
            pass_on(ch, dy).wait_recv()
            upward(ch, share(dy, 1 - c))
        row = lax.broadcasted_iota(jnp.int32, (CR, 128), 0).astype(f32)
        within = row - jnp.floor((row + 0.5) * (1.0 / PAIR)) * PAIR
        parts = []
        for j in range(2):
            gate, up = acc[ch, j, :, 0:128], acc[ch, j, :, 128:256]
            value = gate / (1.0 + jnp.exp(-gate)) * up
            mine = (within >= CAP) if j else (within < CAP)
            parts.append(jnp.where(mine, value, 0.0).astype(bf16))
        act[...] = jnp.concatenate(parts, axis=1)

    def down(s):
        at = pl.ds(pl.multiple_of(s * 512, 512), 512)
        return dot(act[...], dwb.reshape(256, 4096)[:, at])

    def across(ch, dy):
        return remote(xsnd.at[ch, dy], xrcv.at[ch, dy], xs.at[ch, dy], xr.at[ch, dy], pool=partner)

    def home(ch, dy):
        return remote(ssnd.at[ch, dy - 1], rrcv.at[ch, dy - 1], rs.at[ch, dy - 1], rr.at[ch, dy - 1], pool=share(dy, c))

    def lend(ch):
        order = (2, 1, 3, 0)
        values = [down(share(dy, 1 - c)).astype(bf16) for dy in order]
        for dy, value in zip(order, values):
            for b in range(4):
                xsnd[ch, dy, b] = value[:, b * 128 : (b + 1) * 128]
        for dy in order:
            across(ch, dy).start()

    def keep():
        for dy in (2, 1, 3, 0):
            part[dy] = down(share(dy, c))

    def go_home(ch, held, place, ssem, rsem):
        def send_rows(o, carry):
            dx_, dz_ = offset_of(o)
            to = ((ex + dx_) % 4) * 8 + (ez + dz_ + 8) % 8
            remote(
                held.at[:, rows_of(o), :], place.at[:, rows_of(o), :], ssem.at[ch], rsem.at[ch], expert=to
            ).start()
            return carry

        each_offset(ch, send_rows)
        if ch == SELF // CO:
            stays(held, place, rsem)

    def join(ch):
        far = ch in FAR_OUT
        for dy in (1, 3, 2, 0) if far else (2, 1, 3, 0):
            across(ch, dy).wait_recv()
            for b in range(4):
                value = part[dy, :, b * 128 : (b + 1) * 128] + xrcv[ch, dy, b].astype(f32)
                if dy == 2 and far:
                    rsnd2[b, chunk_rows(ch), :] = value.astype(bf16)
                elif dy:
                    ssnd[ch, dy - 1, b] = value.astype(bf16)
                else:
                    fin[b, chunk_rows(ch), :] = value
            if dy == 2 and far:
                go_home(ch, rsnd2, ret2, t2s, t2r)
            elif dy:
                home(ch, dy).start()

    def back(ch):
        for dy in (1, 3) if ch in FAR_OUT else (1, 3, 2):
            home(ch, dy).wait_recv()
        for b in range(4):
            value = fin[b, chunk_rows(ch), :]
            for dy in (1, 3) if ch in FAR_OUT else (1, 2, 3):
                value = value + rrcv[ch, dy - 1, b].astype(f32)
            rsnd[b, chunk_rows(ch), :] = value.astype(bf16)
        go_home(ch, rsnd, ret, ts, tr)

    for ch in range(NCH):
        experts(ch)
        lend(ch)
        if ch + 1 < NCH:
            relay(ch + 1)
        if ch:
            join(ch - 1)
        keep()
        if ch >= 3:
            back(ch - 3)
    join(NCH - 1)
    for ch in range(max(0, NCH - 3), NCH):
        back(ch)

    high = selw[...].astype(bf16)
    low = (selw[...] - high.astype(f32)).astype(bf16)
    both = jnp.concatenate([high, low], axis=0)

    def weigh(place, rows):
        returned = jnp.concatenate([place[b, 0:rows, :] for b in range(4)], axis=1)
        summed = dot(both[:, 0:rows], returned)
        return summed[0:16] + summed[16:32]

    for ch in FAR_OUT:
        wait_bytes(ret2.at[:, chunk_rows(ch), :], t2r.at[ch])
    wsnd[...] = weigh(ret2, len(FAR_OUT) * CR).astype(bf16)
    settle = remote(wsnd, wrcv, ws, wr, pool=across_ring)
    settle.start()
    for ch in range(NCH):
        wait_bytes(ret.at[:, chunk_rows(ch), :], tr.at[ch])
    summed = weigh(ret, ROWS)
    settle.wait_recv()
    fsnd[...] = (hid[...] + (summed + wrcv[...].astype(f32))).astype(bf16)
    local_copy(fsnd, fall.at[p], er).start()

    def send_result(k, carry):
        remote(fsnd, fall.at[p], es, er, pool=(p + k) % POOL).start()
        return carry

    lax.fori_loop(1, POOL, send_result, 0)
    wait_bytes(fall, er)
    for s in range(POOL):
        out[:, s * 512 : (s + 1) * 512] = fall[s]

    swap.wait_send()
    settle.wait_send()
    wait_bytes(qall.at[pl.ds(0, POOL - 1)], qs)
    wait_bytes(psnd.at[pl.ds(0, POOL - 1)], ps)
    wait_bytes(fall.at[pl.ds(0, POOL - 1)], es)
    for k in range(1, 8):
        remote(osnd.at[k - 1], orcv.at[k - 1], os_.at[k - 1], or_.at[k - 1], pool=p).wait_send()
    for ch in range(NCH):
        sent = pl.ds(0, CR - PAIR if ch == SELF // CO else CR)
        wait_bytes(dsnd.at[:, sent, :], ds_.at[ch])
        wait_bytes(rsnd.at[:, sent, :], ts.at[ch])
        if ch in FAR_IN:
            wait_bytes(dsnd2.at[:, sent, :], d2s.at[ch])
        if ch in FAR_OUT:
            wait_bytes(rsnd2.at[:, sent, :], t2s.at[ch])
        for dy in range(4):
            if dy and not (dy == 2 and ch in FAR_IN):
                give(ch, dy).wait_send()
            if dy and not (dy == 2 and ch in FAR_OUT):
                home(ch, dy).wait_send()
            pass_on(ch, dy).wait_send()
            across(ch, dy).wait_send()


def per_device(
    residual, queries, kv_cache, kv_pages, cache_len, page_row, page_len, routes, route_weight,
    out_weight, gate_weight, up_weight, down_weight,
):
    smem = pl.BlockSpec(memory_space=pltpu.SMEM)
    vmem = pl.BlockSpec(memory_space=pltpu.VMEM)
    anywhere = pl.BlockSpec(memory_space=pl.ANY)
    dma = pltpu.SemaphoreType.DMA
    V = pltpu.VMEM
    gathered = pl.pallas_call(
        layer_kernel,
        name="layer",
        out_shape=pltpu.VMEM((16, 4096), bf16),
        in_specs=[smem] * 3 + [anywhere] + [vmem] * 3 + [anywhere] * 6,
        out_specs=vmem,
        scratch_shapes=[
            V((8, 512, 2, 128), bf16),
            V((2, 4, 64, 2, 128), bf16),
            V((512, 4096), bf16),
            V((2, 4096, 128), bf16),
            V((2, 4096, 128), bf16),
            V((2, 128, 4096), bf16),
            V((8, 2, 512), bf16),
            V((8, 8, 8, 128), bf16),
            V((8, 2, 32, 128), bf16),
            V((8, 2, 32, 128), bf16),
            V((8, 8, 128), f32),
            V((8, 8, 128), f32),
            V((8, 8, 128), f32),
            V((8, 8, 128), f32),
            V((64, 128), f32),
            V((7, 16, 512), bf16),
            V((7, 16, 512), bf16),
            V((16, 512), f32),
            V((16, ROWS), f32),
            V((ROWS, 16), bf16),
            V((8, 8, 128), bf16),
            V((4, ROWS, 128), bf16),
            V((8, 4, ROWS, 128), bf16),
            V((NCH, 2, CR, 256), f32),
            V((CR, 256), bf16),
            V((NCH, 4, 4, CR, 128), bf16),
            V((NCH, 4, 4, CR, 128), bf16),
            V((4, CR, 512), f32),
            V((NCH, 3, 4, CR, 128), bf16),
            V((NCH, 3, 4, CR, 128), bf16),
            V((4, ROWS, 128), f32),
            V((4, ROWS, 128), bf16),
            V((4, ROWS, 128), bf16),
            V((16, 512), bf16),
            V((8, 16, 512), bf16),
            V((16, 512), bf16),
            V((16, 512), bf16),
            V((4, ROWS, 128), bf16),
            V((4, ROWS, 128), bf16),
            V((4, ROWS, 128), bf16),
            V((16, 512), bf16),
            V((16, 512), bf16),
            dma((7,)), dma((8,)), dma(()), dma(()), dma(()), dma(()), dma((7,)), dma((7,)),
            dma((NCH,)), dma((NCH,)), dma((NCH, 4)), dma((NCH, 4)), dma((NCH, 4)), dma((NCH, 4)),
            dma((NCH, 4)), dma((NCH, 4)), dma((NCH, 3)), dma((NCH, 3)), dma((NCH,)), dma((NCH,)),
            dma(()), dma(()), dma(()), dma(()), dma((NCH,)), dma((NCH,)), dma((NCH,)), dma((NCH,)), dma(()), dma(()),
        ],
        compiler_params=pltpu.CompilerParams(
            collective_id=0, has_side_effects=True, vmem_limit_bytes=60 * 1024 * 1024
        ),
    )(
        cache_len, page_row.reshape(32), page_len.reshape(32), residual, queries, routes, route_weight,
        kv_cache, kv_pages, out_weight, gate_weight, up_weight, down_weight,
    )
    return gathered.reshape(residual.shape)


def solution(mesh):
    return jax.shard_map(
        per_device,
        mesh=mesh,
        in_specs=(
            P("expert", None, None),
            P("expert", None, "pool", None),
            P("expert", None, None, None, None),
            P("pool", "expert", None, None, None, None),
            P("expert"),
            P(None, "expert"),
            P(None, "expert"),
            P("expert", None, None),
            P("expert", None, None),
            P("pool", None),
            P("expert", None, "pool"),
            P("expert", None, "pool"),
            P("expert", "pool", None),
        ),
        out_specs=P("expert", None, None),
        check_vma=False,
    )
```

```python
import functools
import math

import jax
import jax.numpy as jnp
from jax import lax
from jax.experimental import pallas as pl
from jax.experimental.pallas import tpu as pltpu
from jax.sharding import PartitionSpec as P

very_low = -1e30
MESH = pl.DeviceIdType.MESH
bf16, f32 = jnp.bfloat16, jnp.float32
POOL, EXPERT = 8, 32
CAP = 3
NCH = 4
ROT = 2
FAR_IN = (1, 2, 3)
FAR_OUT = (0, 1, 2)
ROWS = EXPERT * 2 * CAP
CR = ROWS // NCH
CO = EXPERT // NCH
PAIR = 2 * CAP
SELF = (-ROT) % 8 * 4


def local_copy(src, dst, sem):
    return pltpu.make_async_copy(src, dst, sem)


def remote(src, dst, ssem, rsem, **where):
    return pltpu.make_async_remote_copy(
        src_ref=src, dst_ref=dst, send_sem=ssem, recv_sem=rsem, device_id=where, device_id_type=MESH
    )


def wait_bytes(ref, sem):
    pltpu.make_async_copy(ref, ref, sem).wait()


def offset_of(o):
    dzi, dx = (o // 4 + ROT) % 8, o % 4
    return dx, ((dzi + 1) // 2) * (2 * (dzi % 2) - 1)


def dot_t(a, b):
    return lax.dot_general(a, b, (((1,), (1,)), ((), ())), preferred_element_type=f32)


def dot(a, b):
    return jnp.dot(a, b, preferred_element_type=f32)


def layer_kernel(
    clen, prow, plen, res, q, routes, rw, kv, pages, ow, gw, uw, dw,
    out,
    kvb, pgb, owb, gwb, uwb, dwb, resb,
    qall, psnd, prcv, own_m, own_top, own_tot, row_top, att,
    osnd, orcv, hid, selw, picks, q8, dsnd, xg, acc, act,
    xsnd, xrcv, part, ssnd, rrcv, fin, rsnd, ret, fsnd, fall,
    hsnd, hfar, dsnd2, rsnd2, ret2, wsnd, wrcv,
    lsem, kvsem, qs, qr, ps, pr, os_, or_, ds_, dr, as_, ar, fs, fr,
    xs, xr, rs, rr, ts, tr, es, er, gs, gr, d2s, d2r, t2s, t2r, ws, wr,
):
    p = lax.axis_index("pool")
    e = lax.axis_index("expert")
    y, c = p // 2, p % 2
    ex, ez = e // 8, e % 8
    partner = y * 2 + (1 - c)
    head = p // 4
    scale = 1.0 / math.sqrt(128)

    barrier = pltpu.get_barrier_semaphore()

    def greet_pool(k, carry):
        pl.semaphore_signal(barrier, inc=1, device_id={"pool": (p + k) % POOL}, device_id_type=MESH)
        return carry

    def greet_expert(k, carry):
        pl.semaphore_signal(barrier, inc=1, device_id={"expert": (e + k) % EXPERT}, device_id_type=MESH)
        return carry

    lax.fori_loop(1, EXPERT, greet_expert, 0)
    lax.fori_loop(1, POOL, greet_pool, 0)

    for r in range(8):
        local_copy(kv.at[r, :, head], kvb.at[r], kvsem.at[r]).start()
    local_copy(pages.at[:, 0, :, 0], pgb.at[0], lsem.at[0]).start()
    local_copy(pages.at[:, 0, :, 1], pgb.at[1], lsem.at[1]).start()
    own_cols = pl.ds(pl.multiple_of(p * 512, 512), 512)
    local_copy(res.at[:, :, own_cols], resb, lsem.at[2]).start()
    local_copy(ow, owb, lsem.at[3]).start()
    local_copy(gw, gwb, lsem.at[4]).start()
    local_copy(uw, uwb, lsem.at[5]).start()
    local_copy(dw, dwb, lsem.at[6]).start()

    lane = lax.broadcasted_iota(jnp.int32, (16, ROWS), 1).astype(f32)
    spot = jnp.floor((lane + 0.5) * (1.0 / PAIR))
    within = lane - spot * PAIR
    which = jnp.where(within >= CAP, 1.0, 0.0)
    slot = within - which * CAP
    dzi = jnp.floor((spot + 0.5) * 0.25)
    dx = spot - dzi * 4
    dzi = dzi + ROT
    dzi = jnp.where(dzi >= 8, dzi - 8, dzi)
    half = jnp.floor((dzi + 1.5) * 0.5)
    odd = dzi - 2.0 * jnp.floor((dzi + 0.5) * 0.5)
    dz = half * (2.0 * odd - 1.0)
    gx = ex.astype(f32) - dx
    gx = jnp.where(gx < 0, gx + 4, gx)
    gz = ez.astype(f32) - dz
    gz = jnp.where(gz < 0, gz + 8, jnp.where(gz >= 8, gz - 8, gz))
    expert_id = (gx * 8 + gz) * 2 + which
    names = routes[...].reshape(16, 8).astype(f32)
    strengths = rw[...].reshape(16, 8)
    chosen = jnp.zeros((16, ROWS), f32)
    strength = jnp.zeros((16, ROWS), f32)
    for k in range(8):
        hit = names[:, k : k + 1] == expert_id
        chosen = jnp.where(hit, 1.0, chosen)
        strength = jnp.where(hit, strengths[:, k : k + 1], strength)
    earlier = (
        lax.broadcasted_iota(jnp.int32, (16, 16), 1) < lax.broadcasted_iota(jnp.int32, (16, 16), 0)
    ).astype(f32).astype(bf16)
    before = dot(earlier, chosen.astype(bf16))
    taken = jnp.where(before == slot, chosen, 0.0)
    picks[...] = taken.T.astype(bf16)
    selw[...] = taken * strength
    q8[...] = q[...].reshape(8, 8, 128)

    def cache_row(r):
        keys = kvb.reshape(8, 1024, 128)[r]
        s = dot_t(q8[r], keys) * scale
        col = lax.broadcasted_iota(jnp.int32, (8, 1024), 1)
        step = lax.broadcasted_iota(jnp.int32, (8, 1024), 0) // 4
        seen = (col % 2 == 0) & (col <= 2 * (clen[r] + step))
        top = jnp.max(jnp.where(seen, s, very_low), axis=1, keepdims=True)
        w = jnp.where(seen, jnp.exp(s - top), 0.0)
        own_top[r] = jnp.broadcast_to(top, (8, 128))
        own_tot[r] = jnp.broadcast_to(jnp.sum(w, axis=1, keepdims=True), (8, 128))
        own_m[r] = dot(pltpu.roll(w, 1, 1).astype(bf16), keys)

    for r in range(4):
        local_copy(kv.at[r, :, head], kvb.at[r], kvsem.at[r]).wait()
    for r in range(4):
        cache_row(r)

    pl.semaphore_wait(barrier, EXPERT - 1 + POOL - 1)

    peers = [
        ((y + dy) % 4) * 2 + core
        for dy, core in ((2, 1 - c), (2, c), (1, 1 - c), (3, 1 - c), (1, c), (3, c), (0, 1 - c))
    ]
    for to in peers:
        remote(q8, qall.at[p], qs, qr, pool=to).start()
    local_copy(q8, qall.at[p], qr).start()

    for r in range(4, 8):
        local_copy(kv.at[r, :, head], kvb.at[r], kvsem.at[r]).wait()
    for r in range(4, 8):
        cache_row(r)

    local_copy(pages.at[:, 0, :, 0], pgb.at[0], lsem.at[0]).wait()
    local_copy(pages.at[:, 0, :, 1], pgb.at[1], lsem.at[1]).wait()
    wait_bytes(qall, qr)
    scores = []
    for s_ in range(4):
        row = prow[p * 4 + s_]
        for g in range(2):
            asked = jnp.concatenate([qall[4 * g + i, row] for i in range(4)], axis=0)
            scores.append(dot_t(asked, pgb.reshape(2, 4, 128, 128)[g, s_]))
    scores = jnp.concatenate(scores, axis=0) * scale
    lane128 = lax.broadcasted_iota(jnp.int32, (256, 128), 1)
    limit = jnp.concatenate([jnp.full((64, 128), 2 * plen[p * 4 + s_], jnp.int32) for s_ in range(4)], axis=0)
    seen = (lane128 % 2 == 0) & (lane128 < limit)
    top = jnp.max(jnp.where(seen, scores, very_low), axis=1, keepdims=True)
    top = top.astype(bf16).astype(f32)
    w = jnp.where(seen, jnp.exp(scores - top), 0.0)
    total = jnp.sum(w, axis=1, keepdims=True)
    w = pltpu.roll(w, 1, 1).astype(bf16)
    high = total.astype(bf16).astype(f32)
    stats = jnp.where(lane128 < 32, top, jnp.where(lane128 < 64, high, total - high))
    for s_ in range(4):
        for g in range(2):
            at = (s_ * 2 + g) * 32
            mixed = dot(w[at : at + 32], pgb.reshape(2, 4, 128, 128)[g, s_])
            for i in range(4):
                psnd[4 * g + i, 0, s_ * 8 : s_ * 8 + 8] = mixed[i * 8 : i * 8 + 8].astype(bf16)
                psnd[4 * g + i, 1, s_ * 8 : s_ * 8 + 8] = stats[at + i * 8 : at + i * 8 + 8].astype(bf16)

    local_copy(psnd.at[p], prcv.at[p], pr).start()

    for to in peers:
        remote(psnd.at[to], prcv.at[p], ps, pr, pool=to).start()
    local_copy(ow, owb, lsem.at[3]).wait()
    local_copy(res.at[:, :, own_cols], resb, lsem.at[2]).wait()
    wait_bytes(prcv, pr)

    tops = [own_top[r] for r in range(8)]
    match = []
    for n in range(32):
        st = prcv[n // 4, 1, (n % 4) * 8 : (n % 4) * 8 + 8].astype(f32)
        top = jnp.broadcast_to(st[:, 0:1], (8, 128))
        row = prow[n]
        flags = [jnp.where(row == r, 1.0, 0.0) for r in range(8)]
        match.append(flags)
        for r in range(8):
            tops[r] = jnp.maximum(tops[r], top + (flags[r] - 1.0) * 2e30)
    for r in range(8):
        row_top[r] = tops[r]
    nums, dens = [], []
    for r in range(8):
        factor = jnp.exp(own_top[r] - tops[r])
        nums.append(own_m[r] * factor)
        dens.append(own_tot[r] * factor)
    for n in range(32):
        st = prcv[n // 4, 1, (n % 4) * 8 : (n % 4) * 8 + 8].astype(f32)
        top = jnp.broadcast_to(st[:, 0:1], (8, 128))
        total = jnp.broadcast_to(st[:, 32:33] + st[:, 64:65], (8, 128))
        factor = jnp.exp(top - row_top[prow[n]])
        mixed = prcv[n // 4, 0, (n % 4) * 8 : (n % 4) * 8 + 8].astype(f32) * factor
        total = total * factor
        for r in range(8):
            nums[r] = nums[r] + mixed * match[n][r]
            dens[r] = dens[r] + total * match[n][r]
    for r in range(8):
        att[r * 8 : r * 8 + 8] = nums[r] / dens[r]
    attended = jnp.concatenate(
        [att[pl.ds(h, 16, stride=4), :].astype(bf16) for h in range(4)], axis=1
    )

    def project(to):
        return dot(attended, owb[:, pl.ds(pl.multiple_of(to * 512, 512), 512)])

    for k, to in enumerate(peers):
        osnd[k] = project(to).astype(bf16)
        remote(osnd.at[k], orcv.at[k], os_.at[k], or_.at[k], pool=to).start()
    hidden = project(p)
    hidden = hidden + resb[...].reshape(16, 512).astype(f32)
    for k in range(7):
        remote(osnd.at[k], orcv.at[k], os_.at[k], or_.at[k], pool=peers[k]).wait_recv()
        hidden = hidden + orcv[k].astype(f32)
    hid[...] = hidden

    def rows_of(o):
        return pl.ds(o * PAIR, PAIR)

    def chunk_rows(ch):
        return pl.ds(ch * CR, CR)

    def each_offset(ch, body):
        for o in range(ch * CO, (ch + 1) * CO):
            if o != SELF:
                body(o, 0)

    def stays(src, dst, sems):
        rows = pl.ds(SELF * PAIR, PAIR)
        local_copy(src.at[:, rows, :], dst.at[:, rows, :], sems.at[SELF // CO]).start()

    low_hidden = hidden.astype(bf16)
    across_ring = ((y + 2) % 4) * 2 + c
    hsnd[...] = low_hidden
    swap = remote(hsnd, hfar, gs, gr, pool=across_ring)
    swap.start()
    def depart(ch, columns, held, place, ssem, rsem):
        leaving = dot(picks[chunk_rows(ch), :], columns).astype(bf16)
        for b in range(4):
            held[b, chunk_rows(ch), :] = leaving[:, b * 128 : (b + 1) * 128]

        def send_rows(o, carry):
            dx_, dz_ = offset_of(o)
            to = ((ex - dx_ + 4) % 4) * 8 + (ez - dz_ + 8) % 8
            remote(
                held.at[:, rows_of(o), :], xg.at[place, :, rows_of(o), :], ssem.at[ch], rsem.at[ch], expert=to
            ).start()
            return carry

        each_offset(ch, send_rows)
        if ch == SELF // CO:
            stays(held, xg.at[place], rsem)

    for ch in range(NCH):
        depart(ch, low_hidden, dsnd, p, ds_, dr)
    swap.wait_recv()
    for ch in FAR_IN:
        depart(ch, hfar[...], dsnd2, across_ring, d2s, d2r)

    def share(dy, core):
        return ((y + dy) % 4) * 2 + core

    def block_of(s, ch):
        return xg.at[s, :, chunk_rows(ch), :]

    def give(ch, dy):
        to = share(dy, c)
        return remote(block_of(p, ch), block_of(p, ch), as_.at[ch, dy], ar.at[ch, dy], pool=to)

    def pass_on(ch, dy):
        s = share(dy, c)
        return remote(block_of(s, ch), block_of(s, ch), fs.at[ch, dy], fr.at[ch, dy], pool=partner)

    def upward(ch, s, first=False):
        rows = jnp.concatenate([xg[s, b, chunk_rows(ch), :] for b in range(4)], axis=1)
        at = pl.ds(pl.multiple_of(s * 512, 512), 512)
        for j in range(2):
            w = jnp.concatenate([gwb[j, at, :], uwb[j, at, :]], axis=1)
            value = dot(rows, w)
            if first:
                acc[ch, j] = value
            else:
                acc[ch, j] += value

    def offer(ch):
        wait_bytes(block_of(p, ch), dr.at[ch])
        for dy in (1, 3) if ch in FAR_IN else (1, 3, 2):
            give(ch, dy).start()
        pass_on(ch, 0).start()
        upward(ch, p, True)

    local_copy(gw, gwb, lsem.at[4]).wait()
    local_copy(uw, uwb, lsem.at[5]).wait()
    offer(0)
    offer(1)

    local_copy(dw, dwb, lsem.at[6]).wait()

    def relay(ch, then=None):
        for dy in (1, 3, 2):
            if dy == 2 and ch in FAR_IN:
                wait_bytes(block_of(across_ring, ch), d2r.at[ch])
            else:
                give(ch, (4 - dy) % 4).wait_recv()
            pass_on(ch, dy).start()
            if then is not None:
                then(dy)

    def experts(ch):
        pass_on(ch, 0).wait_recv()
        upward(ch, partner)
        if ch == 0:
            relay(ch, lambda dy: upward(ch, share(dy, c)))
            offer(2)
        else:
            for dy in (1, 3, 2):
                upward(ch, share(dy, c))
        for dy in (1, 3, 2):
            pass_on(ch, dy).wait_recv()
            upward(ch, share(dy, 1 - c))
        row = lax.broadcasted_iota(jnp.int32, (CR, 128), 0).astype(f32)
        within = row - jnp.floor((row + 0.5) * (1.0 / PAIR)) * PAIR
        parts = []
        for j in range(2):
            gate, up = acc[ch, j, :, 0:128], acc[ch, j, :, 128:256]
            value = gate / (1.0 + jnp.exp(-gate)) * up
            mine = (within >= CAP) if j else (within < CAP)
            parts.append(jnp.where(mine, value, 0.0).astype(bf16))
        act[...] = jnp.concatenate(parts, axis=1)

    def down(s):
        at = pl.ds(pl.multiple_of(s * 512, 512), 512)
        return dot(act[...], dwb.reshape(256, 4096)[:, at])

    def across(ch, dy):
        return remote(xsnd.at[ch, dy], xrcv.at[ch, dy], xs.at[ch, dy], xr.at[ch, dy], pool=partner)

    def home(ch, dy):
        return remote(ssnd.at[ch, dy - 1], rrcv.at[ch, dy - 1], rs.at[ch, dy - 1], rr.at[ch, dy - 1], pool=share(dy, c))

    def lend(ch):
        order = (2, 1, 3, 0)
        values = [down(share(dy, 1 - c)).astype(bf16) for dy in order]
        for dy, value in zip(order, values):
            for b in range(4):
                xsnd[ch, dy, b] = value[:, b * 128 : (b + 1) * 128]
        for dy in order:
            across(ch, dy).start()

    def keep():
        for dy in (2, 1, 3, 0):
            part[dy] = down(share(dy, c))

    def go_home(ch, held, place, ssem, rsem):
        def send_rows(o, carry):
            dx_, dz_ = offset_of(o)
            to = ((ex + dx_) % 4) * 8 + (ez + dz_ + 8) % 8
            remote(
                held.at[:, rows_of(o), :], place.at[:, rows_of(o), :], ssem.at[ch], rsem.at[ch], expert=to
            ).start()
            return carry

        each_offset(ch, send_rows)
        if ch == SELF // CO:
            stays(held, place, rsem)

    def join(ch):
        far = ch in FAR_OUT
        for dy in (1, 3, 2, 0) if far else (2, 1, 3, 0):
            across(ch, dy).wait_recv()
            for b in range(4):
                value = part[dy, :, b * 128 : (b + 1) * 128] + xrcv[ch, dy, b].astype(f32)
                if dy == 2 and far:
                    rsnd2[b, chunk_rows(ch), :] = value.astype(bf16)
                elif dy:
                    ssnd[ch, dy - 1, b] = value.astype(bf16)
                else:
                    fin[b, chunk_rows(ch), :] = value
            if dy == 2 and far:
                go_home(ch, rsnd2, ret2, t2s, t2r)
            elif dy:
                home(ch, dy).start()

    def back(ch):
        for dy in (1, 3) if ch in FAR_OUT else (1, 3, 2):
            home(ch, dy).wait_recv()
        for b in range(4):
            value = fin[b, chunk_rows(ch), :]
            for dy in (1, 3) if ch in FAR_OUT else (1, 2, 3):
                value = value + rrcv[ch, dy - 1, b].astype(f32)
            rsnd[b, chunk_rows(ch), :] = value.astype(bf16)
        go_home(ch, rsnd, ret, ts, tr)

    for ch in range(NCH):
        experts(ch)
        lend(ch)
        if ch == 0:
            offer(3)
        if ch + 1 < NCH:
            relay(ch + 1)
        if ch:
            join(ch - 1)
        keep()
        if ch >= 3:
            back(ch - 3)
    join(NCH - 1)
    for ch in range(max(0, NCH - 3), NCH):
        back(ch)

    high = selw[...].astype(bf16)
    low = (selw[...] - high.astype(f32)).astype(bf16)
    both = jnp.concatenate([high, low], axis=0)

    def weigh(place, rows):
        returned = jnp.concatenate([place[b, 0:rows, :] for b in range(4)], axis=1)
        summed = dot(both[:, 0:rows], returned)
        return summed[0:16] + summed[16:32]

    for ch in FAR_OUT:
        wait_bytes(ret2.at[:, chunk_rows(ch), :], t2r.at[ch])
    wsnd[...] = weigh(ret2, len(FAR_OUT) * CR).astype(bf16)
    settle = remote(wsnd, wrcv, ws, wr, pool=across_ring)
    settle.start()
    for ch in range(NCH):
        wait_bytes(ret.at[:, chunk_rows(ch), :], tr.at[ch])
    summed = weigh(ret, ROWS)
    settle.wait_recv()
    fsnd[...] = (hid[...] + (summed + wrcv[...].astype(f32))).astype(bf16)
    local_copy(fsnd, fall.at[p], er).start()

    for to in peers:
        remote(fsnd, fall.at[p], es, er, pool=to).start()
    wait_bytes(fall, er)
    for s in range(POOL):
        out[:, s * 512 : (s + 1) * 512] = fall[s]

    swap.wait_send()
    settle.wait_send()
    wait_bytes(qall.at[pl.ds(0, POOL - 1)], qs)
    wait_bytes(psnd.at[pl.ds(0, POOL - 1)], ps)
    wait_bytes(fall.at[pl.ds(0, POOL - 1)], es)
    for k in range(7):
        remote(osnd.at[k], orcv.at[k], os_.at[k], or_.at[k], pool=peers[k]).wait_send()
    for ch in range(NCH):
        sent = pl.ds(0, CR - PAIR if ch == SELF // CO else CR)
        wait_bytes(dsnd.at[:, sent, :], ds_.at[ch])
        wait_bytes(rsnd.at[:, sent, :], ts.at[ch])
        if ch in FAR_IN:
            wait_bytes(dsnd2.at[:, sent, :], d2s.at[ch])
        if ch in FAR_OUT:
            wait_bytes(rsnd2.at[:, sent, :], t2s.at[ch])
        for dy in range(4):
            if dy and not (dy == 2 and ch in FAR_IN):
                give(ch, dy).wait_send()
            if dy and not (dy == 2 and ch in FAR_OUT):
                home(ch, dy).wait_send()
            pass_on(ch, dy).wait_send()
            across(ch, dy).wait_send()


def per_device(
    residual, queries, kv_cache, kv_pages, cache_len, page_row, page_len, routes, route_weight,
    out_weight, gate_weight, up_weight, down_weight,
):
    smem = pl.BlockSpec(memory_space=pltpu.SMEM)
    vmem = pl.BlockSpec(memory_space=pltpu.VMEM)
    anywhere = pl.BlockSpec(memory_space=pl.ANY)
    dma = pltpu.SemaphoreType.DMA
    V = pltpu.VMEM
    gathered = pl.pallas_call(
        layer_kernel,
        name="layer",
        out_shape=pltpu.VMEM((16, 4096), bf16),
        in_specs=[smem] * 3 + [anywhere] + [vmem] * 3 + [anywhere] * 6,
        out_specs=vmem,
        scratch_shapes=[
            V((8, 512, 2, 128), bf16),
            V((2, 4, 64, 2, 128), bf16),
            V((512, 4096), bf16),
            V((2, 4096, 128), bf16),
            V((2, 4096, 128), bf16),
            V((2, 128, 4096), bf16),
            V((8, 2, 512), bf16),
            V((8, 8, 8, 128), bf16),
            V((8, 2, 32, 128), bf16),
            V((8, 2, 32, 128), bf16),
            V((8, 8, 128), f32),
            V((8, 8, 128), f32),
            V((8, 8, 128), f32),
            V((8, 8, 128), f32),
            V((64, 128), f32),
            V((7, 16, 512), bf16),
            V((7, 16, 512), bf16),
            V((16, 512), f32),
            V((16, ROWS), f32),
            V((ROWS, 16), bf16),
            V((8, 8, 128), bf16),
            V((4, ROWS, 128), bf16),
            V((8, 4, ROWS, 128), bf16),
            V((NCH, 2, CR, 256), f32),
            V((CR, 256), bf16),
            V((NCH, 4, 4, CR, 128), bf16),
            V((NCH, 4, 4, CR, 128), bf16),
            V((4, CR, 512), f32),
            V((NCH, 3, 4, CR, 128), bf16),
            V((NCH, 3, 4, CR, 128), bf16),
            V((4, ROWS, 128), f32),
            V((4, ROWS, 128), bf16),
            V((4, ROWS, 128), bf16),
            V((16, 512), bf16),
            V((8, 16, 512), bf16),
            V((16, 512), bf16),
            V((16, 512), bf16),
            V((4, ROWS, 128), bf16),
            V((4, ROWS, 128), bf16),
            V((4, ROWS, 128), bf16),
            V((16, 512), bf16),
            V((16, 512), bf16),
            dma((7,)), dma((8,)), dma(()), dma(()), dma(()), dma(()), dma((7,)), dma((7,)),
            dma((NCH,)), dma((NCH,)), dma((NCH, 4)), dma((NCH, 4)), dma((NCH, 4)), dma((NCH, 4)),
            dma((NCH, 4)), dma((NCH, 4)), dma((NCH, 3)), dma((NCH, 3)), dma((NCH,)), dma((NCH,)),
            dma(()), dma(()), dma(()), dma(()), dma((NCH,)), dma((NCH,)), dma((NCH,)), dma((NCH,)), dma(()), dma(()),
        ],
        compiler_params=pltpu.CompilerParams(
            collective_id=0, has_side_effects=True, vmem_limit_bytes=60 * 1024 * 1024
        ),
    )(
        cache_len, page_row.reshape(32), page_len.reshape(32), residual, queries, routes, route_weight,
        kv_cache, kv_pages, out_weight, gate_weight, up_weight, down_weight,
    )
    return gathered.reshape(residual.shape)


def solution(mesh):
    return jax.shard_map(
        per_device,
        mesh=mesh,
        in_specs=(
            P("expert", None, None),
            P("expert", None, "pool", None),
            P("expert", None, None, None, None),
            P("pool", "expert", None, None, None, None),
            P("expert"),
            P(None, "expert"),
            P(None, "expert"),
            P("expert", None, None),
            P("expert", None, None),
            P("pool", None),
            P("expert", None, "pool"),
            P("expert", None, "pool"),
            P("expert", "pool", None),
        ),
        out_specs=P("expert", None, None),
        check_vma=False,
    )
```

```python
import functools
import math

import jax
import jax.numpy as jnp
from jax import lax
from jax.experimental import pallas as pl
from jax.experimental.pallas import tpu as pltpu
from jax.sharding import PartitionSpec as P

very_low = -1e30
MESH = pl.DeviceIdType.MESH
bf16, f32 = jnp.bfloat16, jnp.float32
POOL, EXPERT = 8, 32
CAP = 3
NCH = 4
ROT = 2
FAR_IN = (0, 1, 2, 3)
FAR_OUT = (0, 1, 2)
ROWS = EXPERT * 2 * CAP
CR = ROWS // NCH
CO = EXPERT // NCH
PAIR = 2 * CAP
SELF = (-ROT) % 8 * 4


def local_copy(src, dst, sem):
    return pltpu.make_async_copy(src, dst, sem)


def remote(src, dst, ssem, rsem, **where):
    return pltpu.make_async_remote_copy(
        src_ref=src, dst_ref=dst, send_sem=ssem, recv_sem=rsem, device_id=where, device_id_type=MESH
    )


def wait_bytes(ref, sem):
    pltpu.make_async_copy(ref, ref, sem).wait()


def offset_of(o):
    dzi, dx = (o // 4 + ROT) % 8, o % 4
    return dx, ((dzi + 1) // 2) * (2 * (dzi % 2) - 1)


def dot_t(a, b):
    return lax.dot_general(a, b, (((1,), (1,)), ((), ())), preferred_element_type=f32)


def dot(a, b):
    return jnp.dot(a, b, preferred_element_type=f32)


def layer_kernel(
    clen, prow, plen, res, q, routes, rw, kv, pages, ow, gw, uw, dw,
    out,
    kvb, pgb, owb, gwb, uwb, dwb, resb,
    qall, psnd, prcv, own_m, own_top, own_tot, row_top, att,
    osnd, orcv, hid, selw, picks, q8, dsnd, xg, acc, act,
    xsnd, xrcv, part, ssnd, rrcv, fin, rsnd, ret, fsnd, fall,
    hsnd, hfar, dsnd2, rsnd2, ret2, wsnd, wrcv,
    lsem, kvsem, qs, qr, ps, pr, os_, or_, ds_, dr, as_, ar, fs, fr,
    xs, xr, rs, rr, ts, tr, es, er, gs, gr, d2s, d2r, t2s, t2r, ws, wr,
):
    p = lax.axis_index("pool")
    e = lax.axis_index("expert")
    y, c = p // 2, p % 2
    ex, ez = e // 8, e % 8
    partner = y * 2 + (1 - c)
    head = p // 4
    scale = 1.0 / math.sqrt(128)

    barrier = pltpu.get_barrier_semaphore()

    def greet_pool(k, carry):
        pl.semaphore_signal(barrier, inc=1, device_id={"pool": (p + k) % POOL}, device_id_type=MESH)
        return carry

    def greet_expert(k, carry):
        pl.semaphore_signal(barrier, inc=1, device_id={"expert": (e + k) % EXPERT}, device_id_type=MESH)
        return carry

    lax.fori_loop(1, EXPERT, greet_expert, 0)
    lax.fori_loop(1, POOL, greet_pool, 0)

    for r in range(8):
        local_copy(kv.at[r, :, head], kvb.at[r], kvsem.at[r]).start()
    local_copy(pages.at[:, 0, :, 0], pgb.at[0], lsem.at[0]).start()
    local_copy(pages.at[:, 0, :, 1], pgb.at[1], lsem.at[1]).start()
    own_cols = pl.ds(pl.multiple_of(p * 512, 512), 512)
    local_copy(res.at[:, :, own_cols], resb, lsem.at[2]).start()
    local_copy(ow, owb, lsem.at[3]).start()
    local_copy(gw, gwb, lsem.at[4]).start()
    local_copy(uw, uwb, lsem.at[5]).start()
    local_copy(dw, dwb, lsem.at[6]).start()

    lane = lax.broadcasted_iota(jnp.int32, (16, ROWS), 1).astype(f32)
    spot = jnp.floor((lane + 0.5) * (1.0 / PAIR))
    within = lane - spot * PAIR
    which = jnp.where(within >= CAP, 1.0, 0.0)
    slot = within - which * CAP
    dzi = jnp.floor((spot + 0.5) * 0.25)
    dx = spot - dzi * 4
    dzi = dzi + ROT
    dzi = jnp.where(dzi >= 8, dzi - 8, dzi)
    half = jnp.floor((dzi + 1.5) * 0.5)
    odd = dzi - 2.0 * jnp.floor((dzi + 0.5) * 0.5)
    dz = half * (2.0 * odd - 1.0)
    gx = ex.astype(f32) - dx
    gx = jnp.where(gx < 0, gx + 4, gx)
    gz = ez.astype(f32) - dz
    gz = jnp.where(gz < 0, gz + 8, jnp.where(gz >= 8, gz - 8, gz))
    expert_id = (gx * 8 + gz) * 2 + which
    names = routes[...].reshape(16, 8).astype(f32)
    strengths = rw[...].reshape(16, 8)
    chosen = jnp.zeros((16, ROWS), f32)
    strength = jnp.zeros((16, ROWS), f32)
    for k in range(8):
        hit = names[:, k : k + 1] == expert_id
        chosen = jnp.where(hit, 1.0, chosen)
        strength = jnp.where(hit, strengths[:, k : k + 1], strength)
    earlier = (
        lax.broadcasted_iota(jnp.int32, (16, 16), 1) < lax.broadcasted_iota(jnp.int32, (16, 16), 0)
    ).astype(f32).astype(bf16)
    before = dot(earlier, chosen.astype(bf16))
    taken = jnp.where(before == slot, chosen, 0.0)
    picks[...] = taken.T.astype(bf16)
    selw[...] = taken * strength
    q8[...] = q[...].reshape(8, 8, 128)

    def cache_row(r):
        keys = kvb.reshape(8, 1024, 128)[r]
        s = dot_t(q8[r], keys) * scale
        col = lax.broadcasted_iota(jnp.int32, (8, 1024), 1)
        step = lax.broadcasted_iota(jnp.int32, (8, 1024), 0) // 4
        seen = (col % 2 == 0) & (col <= 2 * (clen[r] + step))
        top = jnp.max(jnp.where(seen, s, very_low), axis=1, keepdims=True)
        w = jnp.where(seen, jnp.exp(s - top), 0.0)
        own_top[r] = jnp.broadcast_to(top, (8, 128))
        own_tot[r] = jnp.broadcast_to(jnp.sum(w, axis=1, keepdims=True), (8, 128))
        own_m[r] = dot(pltpu.roll(w, 1, 1).astype(bf16), keys)

    for r in range(4):
        local_copy(kv.at[r, :, head], kvb.at[r], kvsem.at[r]).wait()
    for r in range(4):
        cache_row(r)

    pl.semaphore_wait(barrier, EXPERT - 1 + POOL - 1)

    peers = [
        ((y + dy) % 4) * 2 + core
        for dy, core in ((2, 1 - c), (2, c), (1, 1 - c), (3, 1 - c), (1, c), (3, c), (0, 1 - c))
    ]
    for to in peers:
        remote(q8, qall.at[p], qs, qr, pool=to).start()
    local_copy(q8, qall.at[p], qr).start()

    for r in range(4, 8):
        local_copy(kv.at[r, :, head], kvb.at[r], kvsem.at[r]).wait()
    for r in range(4, 8):
        cache_row(r)

    local_copy(pages.at[:, 0, :, 0], pgb.at[0], lsem.at[0]).wait()
    local_copy(pages.at[:, 0, :, 1], pgb.at[1], lsem.at[1]).wait()
    wait_bytes(qall, qr)
    scores = []
    for s_ in range(4):
        row = prow[p * 4 + s_]
        for g in range(2):
            asked = jnp.concatenate([qall[4 * g + i, row] for i in range(4)], axis=0)
            scores.append(dot_t(asked, pgb.reshape(2, 4, 128, 128)[g, s_]))
    scores = jnp.concatenate(scores, axis=0) * scale
    lane128 = lax.broadcasted_iota(jnp.int32, (256, 128), 1)
    limit = jnp.concatenate([jnp.full((64, 128), 2 * plen[p * 4 + s_], jnp.int32) for s_ in range(4)], axis=0)
    seen = (lane128 % 2 == 0) & (lane128 < limit)
    top = jnp.max(jnp.where(seen, scores, very_low), axis=1, keepdims=True)
    top = top.astype(bf16).astype(f32)
    w = jnp.where(seen, jnp.exp(scores - top), 0.0)
    total = jnp.sum(w, axis=1, keepdims=True)
    w = pltpu.roll(w, 1, 1).astype(bf16)
    high = total.astype(bf16).astype(f32)
    stats = jnp.where(lane128 < 32, top, jnp.where(lane128 < 64, high, total - high))
    for s_ in range(4):
        for g in range(2):
            at = (s_ * 2 + g) * 32
            mixed = dot(w[at : at + 32], pgb.reshape(2, 4, 128, 128)[g, s_])
            for i in range(4):
                psnd[4 * g + i, 0, s_ * 8 : s_ * 8 + 8] = mixed[i * 8 : i * 8 + 8].astype(bf16)
                psnd[4 * g + i, 1, s_ * 8 : s_ * 8 + 8] = stats[at + i * 8 : at + i * 8 + 8].astype(bf16)

    local_copy(psnd.at[p], prcv.at[p], pr).start()

    for to in peers:
        remote(psnd.at[to], prcv.at[p], ps, pr, pool=to).start()
    local_copy(ow, owb, lsem.at[3]).wait()
    local_copy(res.at[:, :, own_cols], resb, lsem.at[2]).wait()
    wait_bytes(prcv, pr)

    tops = [own_top[r] for r in range(8)]
    match = []
    for n in range(32):
        st = prcv[n // 4, 1, (n % 4) * 8 : (n % 4) * 8 + 8].astype(f32)
        top = jnp.broadcast_to(st[:, 0:1], (8, 128))
        row = prow[n]
        flags = [jnp.where(row == r, 1.0, 0.0) for r in range(8)]
        match.append(flags)
        for r in range(8):
            tops[r] = jnp.maximum(tops[r], top + (flags[r] - 1.0) * 2e30)
    for r in range(8):
        row_top[r] = tops[r]
    nums, dens = [], []
    for r in range(8):
        factor = jnp.exp(own_top[r] - tops[r])
        nums.append(own_m[r] * factor)
        dens.append(own_tot[r] * factor)
    for n in range(32):
        st = prcv[n // 4, 1, (n % 4) * 8 : (n % 4) * 8 + 8].astype(f32)
        top = jnp.broadcast_to(st[:, 0:1], (8, 128))
        total = jnp.broadcast_to(st[:, 32:33] + st[:, 64:65], (8, 128))
        factor = jnp.exp(top - row_top[prow[n]])
        mixed = prcv[n // 4, 0, (n % 4) * 8 : (n % 4) * 8 + 8].astype(f32) * factor
        total = total * factor
        for r in range(8):
            nums[r] = nums[r] + mixed * match[n][r]
            dens[r] = dens[r] + total * match[n][r]
    for r in range(8):
        att[r * 8 : r * 8 + 8] = nums[r] / dens[r]
    attended = jnp.concatenate(
        [att[pl.ds(h, 16, stride=4), :].astype(bf16) for h in range(4)], axis=1
    )

    def project(to):
        return dot(attended, owb[:, pl.ds(pl.multiple_of(to * 512, 512), 512)])

    for k, to in enumerate(peers):
        osnd[k] = project(to).astype(bf16)
        remote(osnd.at[k], orcv.at[k], os_.at[k], or_.at[k], pool=to).start()
    hidden = project(p)
    hidden = hidden + resb[...].reshape(16, 512).astype(f32)
    for k in range(7):
        remote(osnd.at[k], orcv.at[k], os_.at[k], or_.at[k], pool=peers[k]).wait_recv()
        hidden = hidden + orcv[k].astype(f32)
    hid[...] = hidden

    def rows_of(o):
        return pl.ds(o * PAIR, PAIR)

    def chunk_rows(ch):
        return pl.ds(ch * CR, CR)

    def each_offset(ch, body):
        for o in range(ch * CO, (ch + 1) * CO):
            if o != SELF:
                body(o, 0)

    def stays(src, dst, sems):
        rows = pl.ds(SELF * PAIR, PAIR)
        local_copy(src.at[:, rows, :], dst.at[:, rows, :], sems.at[SELF // CO]).start()

    low_hidden = hidden.astype(bf16)
    across_ring = ((y + 2) % 4) * 2 + c
    hsnd[...] = low_hidden
    swap = remote(hsnd, hfar, gs, gr, pool=across_ring)
    swap.start()
    def depart(ch, columns, held, place, ssem, rsem):
        leaving = dot(picks[chunk_rows(ch), :], columns).astype(bf16)
        for b in range(4):
            held[b, chunk_rows(ch), :] = leaving[:, b * 128 : (b + 1) * 128]

        def send_rows(o, carry):
            dx_, dz_ = offset_of(o)
            to = ((ex - dx_ + 4) % 4) * 8 + (ez - dz_ + 8) % 8
            remote(
                held.at[:, rows_of(o), :], xg.at[place, :, rows_of(o), :], ssem.at[ch], rsem.at[ch], expert=to
            ).start()
            return carry

        each_offset(ch, send_rows)
        if ch == SELF // CO:
            stays(held, xg.at[place], rsem)

    for ch in range(NCH):
        depart(ch, low_hidden, dsnd, p, ds_, dr)
    swap.wait_recv()
    for ch in FAR_IN:
        depart(ch, hfar[...], dsnd2, across_ring, d2s, d2r)

    def share(dy, core):
        return ((y + dy) % 4) * 2 + core

    def block_of(s, ch):
        return xg.at[s, :, chunk_rows(ch), :]

    def give(ch, dy):
        to = share(dy, c)
        return remote(block_of(p, ch), block_of(p, ch), as_.at[ch, dy], ar.at[ch, dy], pool=to)

    def pass_on(ch, dy):
        s = share(dy, c)
        return remote(block_of(s, ch), block_of(s, ch), fs.at[ch, dy], fr.at[ch, dy], pool=partner)

    def upward(ch, s, first=False):
        rows = jnp.concatenate([xg[s, b, chunk_rows(ch), :] for b in range(4)], axis=1)
        at = pl.ds(pl.multiple_of(s * 512, 512), 512)
        for j in range(2):
            w = jnp.concatenate([gwb[j, at, :], uwb[j, at, :]], axis=1)
            value = dot(rows, w)
            if first:
                acc[ch, j] = value
            else:
                acc[ch, j] += value

    def offer(ch):
        wait_bytes(block_of(p, ch), dr.at[ch])
        for dy in (1, 3) if ch in FAR_IN else (1, 3, 2):
            give(ch, dy).start()
        pass_on(ch, 0).start()
        upward(ch, p, True)

    local_copy(gw, gwb, lsem.at[4]).wait()
    local_copy(uw, uwb, lsem.at[5]).wait()
    offer(0)
    offer(1)

    local_copy(dw, dwb, lsem.at[6]).wait()

    def relay(ch, then=None):
        for dy in (1, 3, 2):
            if dy == 2 and ch in FAR_IN:
                wait_bytes(block_of(across_ring, ch), d2r.at[ch])
            else:
                give(ch, (4 - dy) % 4).wait_recv()
            pass_on(ch, dy).start()
            if then is not None:
                then(dy)

    def experts(ch):
        pass_on(ch, 0).wait_recv()
        upward(ch, partner)
        if ch == 0:
            relay(ch, lambda dy: upward(ch, share(dy, c)))
            offer(2)
        else:
            for dy in (1, 3, 2):
                upward(ch, share(dy, c))
        for dy in (1, 3, 2):
            pass_on(ch, dy).wait_recv()
            upward(ch, share(dy, 1 - c))
        row = lax.broadcasted_iota(jnp.int32, (CR, 128), 0).astype(f32)
        within = row - jnp.floor((row + 0.5) * (1.0 / PAIR)) * PAIR
        parts = []
        for j in range(2):
            gate, up = acc[ch, j, :, 0:128], acc[ch, j, :, 128:256]
            value = gate / (1.0 + jnp.exp(-gate)) * up
            mine = (within >= CAP) if j else (within < CAP)
            parts.append(jnp.where(mine, value, 0.0).astype(bf16))
        act[...] = jnp.concatenate(parts, axis=1)

    def down(s):
        at = pl.ds(pl.multiple_of(s * 512, 512), 512)
        return dot(act[...], dwb.reshape(256, 4096)[:, at])

    def across(ch, dy):
        return remote(xsnd.at[ch, dy], xrcv.at[ch, dy], xs.at[ch, dy], xr.at[ch, dy], pool=partner)

    def home(ch, dy):
        return remote(ssnd.at[ch, dy - 1], rrcv.at[ch, dy - 1], rs.at[ch, dy - 1], rr.at[ch, dy - 1], pool=share(dy, c))

    def lend(ch):
        order = (2, 1, 3, 0)
        values = [down(share(dy, 1 - c)).astype(bf16) for dy in order]
        for dy, value in zip(order, values):
            for b in range(4):
                xsnd[ch, dy, b] = value[:, b * 128 : (b + 1) * 128]
        for dy in order:
            across(ch, dy).start()

    def keep():
        for dy in (2, 1, 3, 0):
            part[dy] = down(share(dy, c))

    def go_home(ch, held, place, ssem, rsem):
        def send_rows(o, carry):
            dx_, dz_ = offset_of(o)
            to = ((ex + dx_) % 4) * 8 + (ez + dz_ + 8) % 8
            remote(
                held.at[:, rows_of(o), :], place.at[:, rows_of(o), :], ssem.at[ch], rsem.at[ch], expert=to
            ).start()
            return carry

        each_offset(ch, send_rows)
        if ch == SELF // CO:
            stays(held, place, rsem)

    def join(ch):
        far = ch in FAR_OUT
        for dy in (1, 3, 2, 0) if far else (2, 1, 3, 0):
            across(ch, dy).wait_recv()
            for b in range(4):
                value = part[dy, :, b * 128 : (b + 1) * 128] + xrcv[ch, dy, b].astype(f32)
                if dy == 2 and far:
                    rsnd2[b, chunk_rows(ch), :] = value.astype(bf16)
                elif dy:
                    ssnd[ch, dy - 1, b] = value.astype(bf16)
                else:
                    fin[b, chunk_rows(ch), :] = value
            if dy == 2 and far:
                go_home(ch, rsnd2, ret2, t2s, t2r)
            elif dy:
                home(ch, dy).start()

    def back(ch):
        for dy in (1, 3) if ch in FAR_OUT else (1, 3, 2):
            home(ch, dy).wait_recv()
        for b in range(4):
            value = fin[b, chunk_rows(ch), :]
            for dy in (1, 3) if ch in FAR_OUT else (1, 2, 3):
                value = value + rrcv[ch, dy - 1, b].astype(f32)
            rsnd[b, chunk_rows(ch), :] = value.astype(bf16)
        go_home(ch, rsnd, ret, ts, tr)

    for ch in range(NCH):
        experts(ch)
        lend(ch)
        if ch == 0:
            offer(3)
        if ch + 1 < NCH:
            relay(ch + 1)
        if ch:
            join(ch - 1)
        keep()
        if ch >= 3:
            back(ch - 3)
    join(NCH - 1)
    for ch in range(max(0, NCH - 3), NCH):
        back(ch)

    high = selw[...].astype(bf16)
    low = (selw[...] - high.astype(f32)).astype(bf16)
    both = jnp.concatenate([high, low], axis=0)

    def weigh(place, rows):
        returned = jnp.concatenate([place[b, 0:rows, :] for b in range(4)], axis=1)
        summed = dot(both[:, 0:rows], returned)
        return summed[0:16] + summed[16:32]

    for ch in FAR_OUT:
        wait_bytes(ret2.at[:, chunk_rows(ch), :], t2r.at[ch])
    wsnd[...] = weigh(ret2, len(FAR_OUT) * CR).astype(bf16)
    settle = remote(wsnd, wrcv, ws, wr, pool=across_ring)
    settle.start()
    for ch in range(NCH):
        wait_bytes(ret.at[:, chunk_rows(ch), :], tr.at[ch])
    summed = weigh(ret, ROWS)
    settle.wait_recv()
    fsnd[...] = (hid[...] + (summed + wrcv[...].astype(f32))).astype(bf16)
    local_copy(fsnd, fall.at[p], er).start()

    for to in peers:
        remote(fsnd, fall.at[p], es, er, pool=to).start()
    wait_bytes(fall, er)
    for s in range(POOL):
        out[:, s * 512 : (s + 1) * 512] = fall[s]

    swap.wait_send()
    settle.wait_send()
    wait_bytes(qall.at[pl.ds(0, POOL - 1)], qs)
    wait_bytes(psnd.at[pl.ds(0, POOL - 1)], ps)
    wait_bytes(fall.at[pl.ds(0, POOL - 1)], es)
    for k in range(7):
        remote(osnd.at[k], orcv.at[k], os_.at[k], or_.at[k], pool=peers[k]).wait_send()
    for ch in range(NCH):
        sent = pl.ds(0, CR - PAIR if ch == SELF // CO else CR)
        wait_bytes(dsnd.at[:, sent, :], ds_.at[ch])
        wait_bytes(rsnd.at[:, sent, :], ts.at[ch])
        if ch in FAR_IN:
            wait_bytes(dsnd2.at[:, sent, :], d2s.at[ch])
        if ch in FAR_OUT:
            wait_bytes(rsnd2.at[:, sent, :], t2s.at[ch])
        for dy in range(4):
            if dy and not (dy == 2 and ch in FAR_IN):
                give(ch, dy).wait_send()
            if dy and not (dy == 2 and ch in FAR_OUT):
                home(ch, dy).wait_send()
            pass_on(ch, dy).wait_send()
            across(ch, dy).wait_send()


def per_device(
    residual, queries, kv_cache, kv_pages, cache_len, page_row, page_len, routes, route_weight,
    out_weight, gate_weight, up_weight, down_weight,
):
    smem = pl.BlockSpec(memory_space=pltpu.SMEM)
    vmem = pl.BlockSpec(memory_space=pltpu.VMEM)
    anywhere = pl.BlockSpec(memory_space=pl.ANY)
    dma = pltpu.SemaphoreType.DMA
    V = pltpu.VMEM
    gathered = pl.pallas_call(
        layer_kernel,
        name="layer",
        out_shape=pltpu.VMEM((16, 4096), bf16),
        in_specs=[smem] * 3 + [anywhere] + [vmem] * 3 + [anywhere] * 6,
        out_specs=vmem,
        scratch_shapes=[
            V((8, 512, 2, 128), bf16),
            V((2, 4, 64, 2, 128), bf16),
            V((512, 4096), bf16),
            V((2, 4096, 128), bf16),
            V((2, 4096, 128), bf16),
            V((2, 128, 4096), bf16),
            V((8, 2, 512), bf16),
            V((8, 8, 8, 128), bf16),
            V((8, 2, 32, 128), bf16),
            V((8, 2, 32, 128), bf16),
            V((8, 8, 128), f32),
            V((8, 8, 128), f32),
            V((8, 8, 128), f32),
            V((8, 8, 128), f32),
            V((64, 128), f32),
            V((7, 16, 512), bf16),
            V((7, 16, 512), bf16),
            V((16, 512), f32),
            V((16, ROWS), f32),
            V((ROWS, 16), bf16),
            V((8, 8, 128), bf16),
            V((4, ROWS, 128), bf16),
            V((8, 4, ROWS, 128), bf16),
            V((NCH, 2, CR, 256), f32),
            V((CR, 256), bf16),
            V((NCH, 4, 4, CR, 128), bf16),
            V((NCH, 4, 4, CR, 128), bf16),
            V((4, CR, 512), f32),
            V((NCH, 3, 4, CR, 128), bf16),
            V((NCH, 3, 4, CR, 128), bf16),
            V((4, ROWS, 128), f32),
            V((4, ROWS, 128), bf16),
            V((4, ROWS, 128), bf16),
            V((16, 512), bf16),
            V((8, 16, 512), bf16),
            V((16, 512), bf16),
            V((16, 512), bf16),
            V((4, ROWS, 128), bf16),
            V((4, ROWS, 128), bf16),
            V((4, ROWS, 128), bf16),
            V((16, 512), bf16),
            V((16, 512), bf16),
            dma((7,)), dma((8,)), dma(()), dma(()), dma(()), dma(()), dma((7,)), dma((7,)),
            dma((NCH,)), dma((NCH,)), dma((NCH, 4)), dma((NCH, 4)), dma((NCH, 4)), dma((NCH, 4)),
            dma((NCH, 4)), dma((NCH, 4)), dma((NCH, 3)), dma((NCH, 3)), dma((NCH,)), dma((NCH,)),
            dma(()), dma(()), dma(()), dma(()), dma((NCH,)), dma((NCH,)), dma((NCH,)), dma((NCH,)), dma(()), dma(()),
        ],
        compiler_params=pltpu.CompilerParams(
            collective_id=0, has_side_effects=True, vmem_limit_bytes=60 * 1024 * 1024
        ),
    )(
        cache_len, page_row.reshape(32), page_len.reshape(32), residual, queries, routes, route_weight,
        kv_cache, kv_pages, out_weight, gate_weight, up_weight, down_weight,
    )
    return gathered.reshape(residual.shape)


def solution(mesh):
    return jax.shard_map(
        per_device,
        mesh=mesh,
        in_specs=(
            P("expert", None, None),
            P("expert", None, "pool", None),
            P("expert", None, None, None, None),
            P("pool", "expert", None, None, None, None),
            P("expert"),
            P(None, "expert"),
            P(None, "expert"),
            P("expert", None, None),
            P("expert", None, None),
            P("pool", None),
            P("expert", None, "pool"),
            P("expert", None, "pool"),
            P("expert", "pool", None),
        ),
        out_specs=P("expert", None, None),
        check_vma=False,
    )
```
